256 devices in a mesh: head: 8 (over x, core), batch: 32 (over z, y).
Axes of the slice: x: 4, y: 4, z: 8, core: 2. Of those that a mesh axis runs over, the one named last changes fastest.
Arguments:
- queries: bfloat16 [2048, 4096], P('batch', 'head'), may hold values from -6 to 6
- key_page_cache: bfloat16 [16384, 16, 1024], P('batch', None, 'head'), may hold values from -6 to 6
- value_page_cache: bfloat16 [16384, 16, 1024], P('batch', None, 'head'), may hold values from -6 to 6
- shard_page_index: int32 [32, 512], P('batch'), may hold values from 0 to 511, each once within a row
- sequence_page_count: int32 [32, 64], P('batch'), may hold values from 1 to 64, 512 in all within a row
- last_page_tokens: int32 [2048], P('batch'), may hold values from 1 to 16
- sequence_adapter_entry: int32 [2048], P('batch'), may hold values from 0 to 31
- batch_adapters: int32 [32, 32], P('batch'), may hold values from 0 to 511, as said below
- output_projection_weight: bfloat16 [4096, 4096], P('head'), may hold values from -1.5 to 1.5
- adapter_down_weight: bfloat16 [512, 4096, 64], P('batch', 'head'), may hold values from -1.5 to 1.5
- adapter_up_weight: bfloat16 [512, 64, 4096], P('batch', None, 'head'), may hold values from -0.75 to 0.75
Outputs:
- attention_out: bfloat16 [2048, 4096], P('batch', 'head')
The draws below stay inside these ranges and needn't reach their ends.
Inputs may be any that keep to these rules, and one draw needn't show every extreme that they name: `sequence_page_count`: each row sums to 512. `batch_adapters`: each row holds 32 different ids; at most 2 of a row lie in one aligned range of 16 ids, and exactly 2 in some range; entries may be used by no sequence.
All inputs are finite; a program needn't handle non-finite values.
Results may differ from the reference program's by a relative error of at most 0.013.
Values may be sent and summed in bfloat16 or wider, within the bound.
No kernel may reach another device: no remote copies, remote signals or barrier semaphores. Data moves between devices by JAX's collectives and lax.ppermute only.
A program may use at most 128 MiB of HBM per device.

```python
import math
import jax
import jax.numpy as jnp
import numpy as np
from jax import lax

MODEL_WIDTH = 4096
HQ = 32
KVH = 8
HD = 128
ADAPTER_RANK = 64
ADP_DEV = 16
NEED = 32
PAGE = 16
MAXPG = 64
POOL = 512
SEQ_DEV = 64
SEQS = 2048
ADAPTER_TOTAL = 512
POOL_ALL = 16384
CAP = 2
QUERY_WIDTH = 4096
N_BATCH = 32


def draw_queries(key, part):
    array_extent = (SEQS, HQ, HD)
    values = jnp.clip(jax.random.normal(jax.random.fold_in(key, 1), array_extent, jnp.float32), -6.0, 6.0)
    return values.reshape(SEQS, HQ * HD).astype(jnp.bfloat16)


def draw_key_page_cache(key, part):
    array_extent = (POOL_ALL, PAGE, KVH, HD)
    values = jnp.clip(jax.random.normal(jax.random.fold_in(key, 21), array_extent, jnp.float32), -6.0, 6.0)
    return values.reshape(POOL_ALL, PAGE, KVH * HD).astype(jnp.bfloat16)


def draw_batch_adapters(key, part):
    slots = N_BATCH * CAP

    def shuffle_block(block_key):
        return jax.random.permutation(block_key, ADP_DEV)

    def draw_row(row_key):
        key_order = jax.random.fold_in(row_key, 31)
        key_lead = jax.random.fold_in(row_key, 32)
        key_inner = jax.random.fold_in(row_key, 33)
        order = jax.random.permutation(key_order, slots)
        rank_of = jnp.argsort(order, stable=True).astype(jnp.int32)
        lead = jax.random.randint(key_lead, (), 0, N_BATCH)
        slot_ids = jnp.arange(slots, dtype=jnp.int32)
        block = slot_ids // CAP
        within = slot_ids % CAP
        score = jnp.where(block == lead, within, CAP + rank_of)
        chosen = jnp.argsort(score, stable=True)[:NEED].astype(jnp.int32)
        inner = jax.vmap(shuffle_block)(jax.random.split(key_inner, N_BATCH)).astype(jnp.int32)
        chosen_block = chosen // CAP
        return (chosen_block * ADP_DEV + inner[chosen_block, chosen % CAP]).astype(jnp.int32)
    return jax.vmap(draw_row)(jax.random.split(jax.random.fold_in(key, 30), N_BATCH))


def place_ends(drawn, rng, low, top_value):
    index_at = [jax.random.randint(jax.random.fold_in(rng, axis), (), 0, length) for axis, length in enumerate(drawn.shape)]
    widest = drawn.shape.index(max(drawn.shape))
    beside = index_at[:widest] + [(index_at[widest] + 1) % drawn.shape[widest]] + index_at[widest + 1:]
    return drawn.at[tuple(index_at)].set(low).at[tuple(beside)].set(top_value)


def level_of(rng, shape, cuts, least, largest):
    def one(position, shards_of):
        steps = jax.random.uniform(jax.random.fold_in(jax.random.fold_in(rng, 6), position), (shards_of,), jnp.float32, least / len(cuts), largest / len(cuts))
        return jnp.repeat(jnp.exp(steps), shape[position] // shards_of).reshape((-1,) + (1,) * (len(shape) - position - 1))

    gain = one(*cuts[0])
    for cut in cuts[1:]:
        gain = gain * one(*cut)
    return gain


def length_profile(amount, total, limit, slope):
    portions = [(1 << 20) // math.isqrt(standing ** slope) + 1 for standing in range(2, amount + 1)]
    rest, given = total - limit - (amount - 1), [1] * (amount - 1)
    while rest > 0:
        movable = [i for i in range(amount - 1) if given[i] < limit]
        whole, remaining = sum([portions[i] for i in movable]), rest
        for i in movable:
            addition = min(limit - given[i], max(1, remaining * portions[i] // whole), rest)
            given[i] = given[i] + addition
            rest = rest - addition
    return np.array([limit] + given)


def uneven_parts(rng, amount, total, bound, skew):
    if amount == 2:
        one = jax.random.randint(rng, (), max(1, total - bound), min(bound, total - 1) + 1)
        return jnp.stack([one, total - one])
    lengths = jnp.asarray(length_profile(amount, total, bound, skew), jnp.int32)
    twos = (amount - 1) // 2
    source_of, receiver = lengths[1:1 + 2 * twos:2], lengths[2:2 + 2 * twos:2]
    margin = jnp.minimum(source_of - 1, bound - receiver)
    passed = jax.random.randint(jax.random.fold_in(rng, 1), (twos,), 0, 1 << 20) % (margin + 1)
    lengths = lengths.at[1:1 + 2 * twos:2].set(source_of - passed).at[2:2 + 2 * twos:2].set(receiver + passed)
    return lengths[jax.random.permutation(jax.random.fold_in(rng, 2), amount)]


def bell_draw(key, extent, spread, bound, shards=(), kind=jnp.bfloat16):
    entries = spread * jax.random.normal(key, extent, jnp.float32)
    if shards:
        entries = entries * level_of(key, extent, shards, -0.22, 0.18)
    return jnp.clip(entries, -bound, bound).astype(kind)


def setup_inputs(seed: int = 0) -> dict:
    streams_of = jax.random.split(jax.random.key(seed), 12)
    queries = draw_queries(jax.random.fold_in(streams_of[11], 71), 0)
    key_page_cache = draw_key_page_cache(jax.random.fold_in(streams_of[11], 71), 0)
    value_page_cache = bell_draw(streams_of[2], (POOL_ALL, PAGE, KVH * HD), 1.0, 6.0, ((0, 32), (2, 8)))
    shard_page_index = jax.vmap(lambda own: jax.random.permutation(own, POOL))(jax.random.split(streams_of[3], N_BATCH)).reshape((N_BATCH, POOL)).astype(jnp.int32)
    sequence_page_count = jax.vmap(lambda own: uneven_parts(own, SEQ_DEV, POOL, MAXPG, 2))(jax.random.split(streams_of[4], N_BATCH)).reshape((N_BATCH, SEQ_DEV)).astype(jnp.int32)
    last_page_tokens = place_ends(jax.random.randint(streams_of[5], (SEQS,), 1, PAGE + 1), jax.random.fold_in(streams_of[5], 1), 1, PAGE).astype(jnp.int32)
    sequence_adapter_entry = place_ends(jax.random.randint(streams_of[6], (SEQS,), 0, NEED), jax.random.fold_in(streams_of[6], 1), 0, NEED - 1).astype(jnp.int32)
    batch_adapters = draw_batch_adapters(jax.random.fold_in(streams_of[11], 71), 0)
    output_projection_weight = bell_draw(streams_of[8], (QUERY_WIDTH, MODEL_WIDTH), (QUERY_WIDTH // 256) ** -0.5, 1.5, ((0, 8),))
    adapter_down_weight = bell_draw(streams_of[9], (ADAPTER_TOTAL, QUERY_WIDTH, ADAPTER_RANK), (QUERY_WIDTH // 256) ** -0.5, 1.5, ((0, 32), (1, 8)))
    adapter_up_weight = bell_draw(streams_of[10], (ADAPTER_TOTAL, ADAPTER_RANK, MODEL_WIDTH), ADAPTER_RANK ** -0.5, 0.75, ((0, 32), (2, 8)))
    return dict(queries=queries, key_page_cache=key_page_cache, value_page_cache=value_page_cache, shard_page_index=shard_page_index, sequence_page_count=sequence_page_count, last_page_tokens=last_page_tokens, sequence_adapter_entry=sequence_adapter_entry, batch_adapters=batch_adapters, output_projection_weight=output_projection_weight, adapter_down_weight=adapter_down_weight, adapter_up_weight=adapter_up_weight)


def attend(queries, keys, values, shard_page_index, sequence_page_count, last_page_tokens):
    rows = queries.shape[0]
    kv_heads = keys.shape[2] // HD
    groups = HQ // KVH
    page_start = jnp.cumsum(sequence_page_count) - sequence_page_count
    positions = jnp.arange(MAXPG, dtype=jnp.int32)
    slot_index = jnp.minimum(page_start[:, None] + positions[None, :], shard_page_index.shape[0] - 1).astype(jnp.int32)
    page_ids = jnp.take(shard_page_index, slot_index, axis=0).astype(jnp.int32)
    key_rows = jnp.take(keys, page_ids, axis=0).reshape(rows, MAXPG * PAGE, kv_heads, HD)
    value_rows = jnp.take(values, page_ids, axis=0).reshape(rows, MAXPG * PAGE, kv_heads, HD)
    grouped = queries.reshape(rows, kv_heads, groups, HD)
    scores = jnp.einsum("skgd,stkd->skgt", grouped.astype(jnp.float32), key_rows.astype(jnp.float32)) * (HD ** -0.5)
    context = (sequence_page_count - 1) * PAGE + last_page_tokens
    live_mask = jnp.arange(MAXPG * PAGE, dtype=jnp.int32)[None, :] < context[:, None]
    scores = jnp.where(live_mask[:, None, None, :], scores, -1e30)
    top_score = jnp.max(scores, axis=-1, keepdims=True)
    powers = jnp.exp(scores - top_score)
    weights = (powers / jnp.sum(powers, axis=-1, keepdims=True)).astype(jnp.bfloat16)
    weights = lax.optimization_barrier(weights)
    mixed = jnp.einsum("skgt,stkd->skgd", weights.astype(jnp.float32), value_rows.astype(jnp.float32))
    return mixed.astype(jnp.bfloat16).reshape(rows, kv_heads * groups * HD)


def reference(queries, key_page_cache, value_page_cache, shard_page_index, sequence_page_count, last_page_tokens, sequence_adapter_entry, batch_adapters, output_projection_weight, adapter_down_weight, adapter_up_weight):
    def shard_step(packed):
        query_b, key_b, value_b, order_b, count_b, fill_b, slot_b, list_b = packed
        attention = attend(query_b, key_b, value_b, order_b, count_b, fill_b)
        attention = lax.optimization_barrier(attention)
        base = jnp.dot(attention, output_projection_weight, preferred_element_type=jnp.float32)
        adapter_numbers = jnp.take(list_b, slot_b, axis=0).astype(jnp.int32)
        down_matrix_rows = jnp.take(adapter_down_weight, adapter_numbers, axis=0).astype(jnp.float32)
        reduced = jnp.einsum("sk,skr->sr", attention.astype(jnp.float32), down_matrix_rows)
        ranked = lax.optimization_barrier(reduced.astype(jnp.bfloat16))
        up_matrix_rows = jnp.take(adapter_up_weight, adapter_numbers, axis=0).astype(jnp.float32)
        grown = jnp.einsum("sr,src->sc", ranked.astype(jnp.float32), up_matrix_rows)
        return (base + grown).astype(jnp.bfloat16)

    packed = (
        queries.reshape(N_BATCH, SEQ_DEV, QUERY_WIDTH),
        key_page_cache.reshape(N_BATCH, POOL, PAGE, KVH * HD),
        value_page_cache.reshape(N_BATCH, POOL, PAGE, KVH * HD),
        shard_page_index,
        sequence_page_count,
        last_page_tokens.reshape(N_BATCH, SEQ_DEV),
        sequence_adapter_entry.reshape(N_BATCH, SEQ_DEV),
        batch_adapters,
    )
    return lax.map(shard_step, packed).reshape(SEQS, MODEL_WIDTH)
```

```python
import jax
import jax.numpy as jnp
from jax import lax
from jax.sharding import PartitionSpec as P

HQ = 32
KVH = 8
HD = 128
PAGE = 16
BLOCK = 16
HOME_ROWS = 128


def from_everyone(shard, axis):
    count = lax.axis_size(axis)
    return lax.all_to_all(
        jnp.broadcast_to(shard[None], (count, *shard.shape)), axis, 0, 0, tiled=True
    )


def joined_along(blocks, dim):
    blocks = jnp.moveaxis(blocks, 0, dim)
    dims = blocks.shape
    return blocks.reshape(*dims[:dim], dims[dim] * dims[dim + 1], *dims[dim + 2 :])


def collect(shard, axis, dim):
    blocks = from_everyone(shard, axis)
    return joined_along(blocks, dim)


def attend(queries, keys, values, shard_page_index, sequence_page_count, last_page_tokens):
    rows = queries.shape[0]
    pool_pages = keys.shape[0]
    kv_heads = keys.shape[2] // HD
    groups = HQ // KVH
    page_start = jnp.cumsum(sequence_page_count) - sequence_page_count
    pool_range = jnp.arange(pool_pages, dtype=jnp.int32)
    place_match = shard_page_index[:, None] == pool_range[None, :]
    page_place = jnp.sum(jnp.where(place_match, pool_range[:, None], 0), axis=0)
    token_place = (page_place[:, None] * PAGE + jnp.arange(PAGE, dtype=jnp.int32)[None, :]).reshape(
        pool_pages * PAGE
    )
    key_flat = keys.reshape(pool_pages * PAGE, kv_heads, HD)
    value_flat = values.reshape(pool_pages * PAGE, kv_heads, HD)
    grouped = queries.reshape(rows, kv_heads, groups, HD)
    scores = jnp.einsum(
        "skgd,tkd->skgt", grouped, key_flat, preferred_element_type=jnp.float32
    ) * HD ** (-0.5)
    context = (sequence_page_count - 1) * PAGE + last_page_tokens
    lower = page_start * PAGE
    live_mask = (token_place[None, :] >= lower[:, None]) & (
        token_place[None, :] < (lower + context)[:, None]
    )
    scores = jnp.where(live_mask[:, None, None, :], scores, -1e30)
    top_score = jnp.max(scores, axis=-1, keepdims=True)
    powers = jnp.exp(scores - top_score)
    weights = (powers / jnp.sum(powers, axis=-1, keepdims=True)).astype(jnp.bfloat16)
    mixed = jnp.einsum("skgt,tkd->skgd", weights, value_flat, preferred_element_type=jnp.float32)
    return mixed.astype(jnp.bfloat16).reshape(rows, kv_heads * groups * HD)


def exchange(blocks, axis):
    return lax.all_to_all(blocks, axis, split_axis=0, concat_axis=0, tiled=True)


def grown_by_moving_maps(
    attention, sequence_adapter_entry, batch_adapters, adapter_down_weight, adapter_up_weight
):
    rows = attention.shape[0]
    my_index = lax.axis_index("batch")
    peers = lax.axis_size("batch")
    count_each_shard = adapter_down_weight.shape[0]
    adapter_rank_width = adapter_down_weight.shape[2]
    output_width = adapter_up_weight.shape[2]
    need = batch_adapters.shape[1]
    own_list = batch_adapters[0]
    slot_match = sequence_adapter_entry[:, None] == jnp.arange(need, dtype=jnp.int32)[None, :]
    lists = collect(batch_adapters, "batch", 0)
    slot_cap = 2 * need // peers
    mine = (lists // count_each_shard == my_index).astype(jnp.int32)
    before = jnp.cumsum(mine, axis=1) - mine
    slot_range = jnp.arange(slot_cap, dtype=jnp.int32)
    select = (mine[:, None, :] == 1) & (before[:, None, :] == slot_range[None, :, None])
    shard_local_numbers = jnp.sum(
        jnp.where(select, (lists % count_each_shard)[:, None, :], 0), axis=-1
    )
    filled = jnp.any(select, axis=-1)
    stored_range = jnp.arange(count_each_shard, dtype=jnp.int32)
    one_hot = (
        (shard_local_numbers[:, :, None] == stored_range[None, None, :]) & filled[:, :, None]
    ).astype(jnp.bfloat16)
    send_shrink = jnp.einsum(
        "bcn,nkr->bckr", one_hot, adapter_down_weight, preferred_element_type=jnp.float32
    ).astype(jnp.bfloat16)
    send_expand = jnp.einsum(
        "bcn,nrw->bcrw", one_hot, adapter_up_weight, preferred_element_type=jnp.float32
    ).astype(jnp.bfloat16)
    got_shrink, got_expand = exchange(send_shrink, "batch"), exchange(send_expand, "batch")
    my_home = own_list // count_each_shard
    order_range = jnp.arange(need, dtype=jnp.int32)
    same_home = (my_home[:, None] == my_home[None, :]) & (
        order_range[None, :] < order_range[:, None]
    )
    arrival = my_home * slot_cap + jnp.sum(same_home, axis=1)
    seq_arrival = jnp.sum(jnp.where(slot_match, arrival[None, :], 0), axis=1)
    total_slots = peers * slot_cap
    picked = seq_arrival[:, None] == jnp.arange(total_slots, dtype=jnp.int32)[None, :]
    flat_shrink = got_shrink.reshape(total_slots, got_shrink.shape[2], adapter_rank_width)
    per_slot = jnp.einsum("sk,nkr->snr", attention, flat_shrink, preferred_element_type=jnp.float32)
    shrink_part = jnp.sum(per_slot * picked.astype(jnp.float32)[:, :, None], axis=1)
    ranked = lax.psum(shrink_part, "head").astype(jnp.bfloat16)
    spread = (ranked[:, None, :] * picked.astype(jnp.bfloat16)[:, :, None]).reshape(
        rows, total_slots * adapter_rank_width
    )
    return jnp.dot(
        spread,
        got_expand.reshape(total_slots * adapter_rank_width, output_width),
        preferred_element_type=jnp.float32,
    )


def per_device(
    queries,
    key_page_cache,
    value_page_cache,
    shard_page_index,
    sequence_page_count,
    last_page_tokens,
    sequence_adapter_entry,
    batch_adapters,
    output_projection_weight,
    adapter_down_weight,
    adapter_up_weight,
):
    f32, bf16, i32 = jnp.float32, jnp.bfloat16, jnp.int32
    rows, width = queries.shape
    peers = lax.axis_size("batch")
    heads = lax.axis_size("head")
    stored, _, rank_width = adapter_down_weight.shape
    need = batch_adapters.shape[1]
    output_width = adapter_up_weight.shape[2]
    slots = peers * BLOCK

    own_list = batch_adapters[0]
    listed = sequence_adapter_entry[:, None] == jnp.arange(need, dtype=i32)[None, :]
    ids = jnp.sum(jnp.where(listed, own_list[None, :], 0), axis=1)
    home, local = ids // stored, ids % stored
    order = jnp.arange(rows, dtype=i32)
    place = jnp.sum((home[:, None] == home[None, :]) & (order[None, :] < order[:, None]), axis=1, dtype=i32)
    fits = place < BLOCK - 1
    slot = jnp.where(fits, home * BLOCK + place, -1)
    pair_over = jnp.any(~fits)
    picked = jnp.arange(slots, dtype=i32)[:, None] == slot[None, :]
    slot_local = jnp.sum(jnp.where(picked, local[None, :] + 1, 0), axis=1).reshape(peers, BLOCK)
    lane = jnp.arange(BLOCK, dtype=i32)
    header = jnp.where(lane[None, :] == BLOCK - 1, pair_over.astype(i32), slot_local)
    header = jnp.pad(header, ((0, 0), (0, width - BLOCK))).astype(bf16)

    attention = attend(
        queries,
        key_page_cache,
        value_page_cache,
        shard_page_index[0],
        sequence_page_count[0],
        last_page_tokens,
    )
    send = jnp.dot(picked.astype(bf16), attention, preferred_element_type=f32).astype(bf16)
    send = send.reshape(peers, BLOCK, width)
    send = jnp.where(lane[None, :, None] == BLOCK - 1, header[:, None, :], send)
    got = exchange(send, "batch")

    base_part = jnp.dot(attention, output_projection_weight, preferred_element_type=f32).astype(bf16)
    got_header = got[:, BLOCK - 1, :BLOCK].astype(f32).astype(i32)
    any_pair_over = jnp.max(got_header[:, BLOCK - 1]) > 0
    got_local = jnp.where(lane[None, :] == BLOCK - 1, 0, got_header).reshape(slots) - 1
    filled = got_local >= 0
    upto = jnp.arange(slots, dtype=i32)
    at = jnp.sum((upto[None, :] < upto[:, None]) & filled[None, :], axis=1, dtype=i32)
    home_over = jnp.sum(filled, dtype=i32) > HOME_ROWS
    at = jnp.where(filled, at, -1)
    closing = jnp.arange(HOME_ROWS, dtype=i32)[:, None] == at[None, :]
    closed = jnp.dot(closing.astype(bf16), got.reshape(slots, width), preferred_element_type=f32).astype(bf16)
    row_local = jnp.sum(jnp.where(closing, got_local[None, :], 0), axis=1)
    uses = row_local[:, None] == jnp.arange(stored, dtype=i32)[None, :]
    per_map = jnp.einsum("mk,nkr->mnr", closed, adapter_down_weight, preferred_element_type=f32)
    part = jnp.sum(per_map * uses.astype(f32)[:, :, None], axis=1)
    half = HOME_ROWS // 2
    packed = jnp.concatenate([part[:half], part[half:]], axis=1).astype(bf16)

    parts = jnp.concatenate(
        [
            jnp.moveaxis(base_part.reshape(rows, heads, output_width), 1, 0),
            jnp.broadcast_to(packed[None], (heads, *packed.shape)),
        ],
        axis=2,
    )
    parts = exchange(parts, "head")
    summed = jnp.sum(parts.astype(f32), axis=0)
    base = summed[:, :output_width]
    ranked = jnp.concatenate(
        [summed[:, output_width : output_width + rank_width], summed[:, output_width + rank_width :]], axis=0
    ).astype(bf16)
    spread = (ranked[:, None, :] * uses.astype(bf16)[:, :, None]).reshape(HOME_ROWS, stored * rank_width)
    grown_home = jnp.dot(
        spread, adapter_up_weight.reshape(stored * rank_width, output_width), preferred_element_type=f32
    ).astype(bf16)
    back = jnp.einsum("ms,mw->sw", closing.astype(bf16), grown_home, preferred_element_type=f32).astype(bf16)
    back = back.reshape(peers, BLOCK, output_width)
    back = jnp.where(lane[None, :, None] == BLOCK - 1, home_over.astype(bf16), back)
    back = exchange(back, "batch")

    any_home_over = jnp.max(back[:, BLOCK - 1, 0].astype(f32)) > 0
    grown = jnp.einsum(
        "sr,sw->rw", picked.astype(bf16), back.reshape(slots, output_width), preferred_element_type=f32
    )
    grown = lax.cond(
        any_pair_over | any_home_over,
        lambda: grown_by_moving_maps(
            attention, sequence_adapter_entry, batch_adapters, adapter_down_weight, adapter_up_weight
        ),
        lambda: grown,
    )
    return (base + grown).astype(bf16)


def solution(mesh):
    in_specs = (
        P("batch", "head"),
        P("batch", None, "head"),
        P("batch", None, "head"),
        P("batch", None),
        P("batch", None),
        P("batch"),
        P("batch"),
        P("batch", None),
        P("head", None),
        P("batch", "head", None),
        P("batch", None, "head"),
    )
    out_specs = P("batch", "head")
    return jax.shard_map(
        per_device, mesh=mesh, in_specs=in_specs, out_specs=out_specs, check_vma=False
    )
```

```python
import functools

import jax
import jax.numpy as jnp
from jax import lax
from jax.experimental import pallas as pl
from jax.experimental.pallas import tpu as pltpu
from jax.sharding import PartitionSpec as P

HQ = 32
KVH = 8
HD = 128
PAGE = 16
BLOCK = 16
HOME_ROWS = 128
CHUNK = 512
F32, BF16, I32 = jnp.float32, jnp.bfloat16, jnp.int32


def iota(shape, dim):
    return lax.broadcasted_iota(I32, shape, dim)


def nn(a, b):
    return lax.dot_general(a, b, (((1,), (0,)), ((), ())), preferred_element_type=F32)


def nt(a, b):
    return lax.dot_general(a, b, (((1,), (1,)), ((), ())), preferred_element_type=F32)


def column(row):
    n = row.shape[1]
    return jnp.sum(jnp.where(iota((n, n), 0) == iota((n, n), 1), row, 0.0), axis=1, keepdims=True)


def source_kernel(
    index_ref,
    count_ref,
    last_ref,
    entry_ref,
    list_ref,
    q_ref,
    keys_hbm,
    values_hbm,
    send_ref,
    attention_ref,
    target_ref,
    keys_ref,
    values_ref,
    scores_ref,
    owner_ref,
    sems,
    *,
    stored,
    peers,
):
    rows = q_ref.shape[0]
    pages = index_ref.shape[1]
    tokens = pages * PAGE
    groups = HQ // KVH
    steps = tokens // CHUNK
    copy_keys = pltpu.make_async_copy(keys_hbm, keys_ref, sems.at[0])
    copy_values = pltpu.make_async_copy(values_hbm, values_ref, sems.at[1])
    copy_keys.start()
    copy_values.start()

    count = count_ref[...].astype(F32)
    end = jnp.sum(jnp.where(iota((rows, rows), 1) <= iota((rows, rows), 0), count, 0.0), axis=1, keepdims=True)
    last = column(last_ref[...].astype(F32))
    position = iota((rows, pages), 1).astype(F32)
    owner = jnp.sum((end <= position).astype(F32), axis=0, keepdims=True)
    limit = PAGE - jnp.sum(jnp.where(position == end - 1.0, PAGE - last, 0.0), axis=0, keepdims=True)
    index = index_ref[...]
    per_row = 128 // PAGE
    high = iota((tokens // 128, pages), 0) == index // per_row
    low = (iota((128, pages), 0) // PAGE == index % per_row).astype(F32).astype(BF16)
    owner = nt(jnp.where(high, owner, 0.0).astype(BF16), low)
    limit = nt(jnp.where(high, limit, 0.0).astype(BF16), low)
    inside = (iota((tokens // 128, 128), 1) % PAGE).astype(F32) < limit
    owner_ref[...] = jnp.where(inside, owner, -1.0)

    adapters = list_ref[...].astype(F32)
    entry = entry_ref[...].astype(F32)
    need = adapters.shape[1]
    ids_row = jnp.sum(
        jnp.where(iota((need, rows), 0).astype(F32) == entry, column(adapters), 0.0), axis=0, keepdims=True
    )
    ids_col = column(ids_row)
    home_row = ids_row.astype(I32) // stored
    home_col = ids_col.astype(I32) // stored
    local_row = ids_row.astype(I32) % stored
    same = home_col == home_row
    sub, lane = iota((rows, rows), 0), iota((rows, rows), 1)
    place_row = jnp.sum((same & (sub < lane)).astype(F32), axis=0, keepdims=True).astype(I32)
    place_col = jnp.sum((same & (lane < sub)).astype(F32), axis=1, keepdims=True).astype(I32)
    target = jnp.where(place_row < BLOCK - 1, home_row * BLOCK + place_row, -1)
    target_ref[...] = target
    over = jnp.max(place_row.astype(F32), axis=1, keepdims=True) >= BLOCK - 1
    width = q_ref.shape[1]
    heads_of = jnp.where(iota((peers, rows), 0) == home_row, local_row + 1, 0).astype(F32).astype(BF16)
    spread = (iota((rows, width), 1) % BLOCK == place_col).astype(F32).astype(BF16)
    header = nn(heads_of, spread)
    header = jnp.where(iota((peers, width), 1) % BLOCK == BLOCK - 1, over.astype(F32), header).astype(BF16)

    q = jnp.concatenate([q_ref[:, g * HD : (g + 1) * HD] for g in range(groups)], axis=0)
    own = (iota((groups * rows, 128), 0) % rows).astype(F32)
    copy_keys.wait()
    top = jnp.full((groups * rows, 128), -1e30, F32)
    for step in range(steps):
        block = nt(q, keys_ref[step * CHUNK : (step + 1) * CHUNK, :])
        for part in range(CHUNK // 128):
            at = step * (CHUNK // 128) + part
            kept = jnp.where(owner_ref[at : at + 1, :] == own, block[:, part * 128 : (part + 1) * 128], -1e30)
            scores_ref[:, at * 128 : (at + 1) * 128] = kept
            top = jnp.maximum(top, kept)
    factor = HD**-0.5 * 1.4426950408889634
    top = jnp.max(top, axis=1, keepdims=True)
    copy_values.wait()
    total = jnp.zeros((groups * rows, 128), F32)
    mixed = jnp.zeros((groups * rows, HD), F32)
    for step in range(steps):
        powers = jnp.exp2((scores_ref[:, step * CHUNK : (step + 1) * CHUNK] - top) * factor)
        for part in range(CHUNK // 128):
            total = total + powers[:, part * 128 : (part + 1) * 128]
        mixed = mixed + nn(powers.astype(BF16), values_ref[step * CHUNK : (step + 1) * CHUNK, :])
    mixed = (mixed / jnp.sum(total, axis=1, keepdims=True)).astype(BF16)
    attention = jnp.concatenate([mixed[g * rows : (g + 1) * rows] for g in range(groups)], axis=1)
    attention_ref[...] = attention

    slots = peers * BLOCK
    picked = jnp.concatenate(
        [
            (iota((slots, rows), 0) == target).astype(F32),
            (iota((slots, peers), 0) == iota((slots, peers), 1) * BLOCK + BLOCK - 1).astype(F32),
        ],
        axis=1,
    ).astype(BF16)
    send_ref[...] = nn(picked, jnp.concatenate([attention, header], axis=0)).astype(BF16)


def base_kernel(attention_ref, weight_ref, out_ref):
    out_ref[0] = nn(attention_ref[...], weight_ref[...]).astype(BF16)


def home_down_kernel(got_ref, down_ref, base_ref, parts_ref, closing_ref, local_ref, over_ref):
    slots, width = got_ref.shape
    peers = slots // BLOCK
    got = got_ref[...]
    is_header = (iota((peers, slots), 1) == iota((peers, slots), 0) * BLOCK + BLOCK - 1).astype(F32).astype(BF16)
    header = nn(is_header, got)[:, :slots]
    lane = iota((peers, slots), 1)
    sub = iota((peers, slots), 0)
    flags = jnp.where(lane % BLOCK == BLOCK - 1, header, 0.0)
    ids = jnp.where(lane % BLOCK == BLOCK - 1, 0.0, header)
    ids_first = jnp.where(lane < BLOCK, ids, 0.0)
    filled = jnp.sum((ids_first > 0.0).astype(F32), axis=1, keepdims=True)
    before = jnp.sum(jnp.where(sub < lane // BLOCK, filled, 0.0), axis=0, keepdims=True)
    here = jnp.sum(jnp.where(sub == lane // BLOCK, filled, 0.0), axis=0, keepdims=True)
    local = jnp.sum(jnp.where(sub == lane // BLOCK, ids, 0.0), axis=0, keepdims=True)
    within = (iota((1, slots), 1) % BLOCK).astype(F32)
    at = jnp.where(within < here, before + within, -1.0)
    closing = (at == iota((HOME_ROWS, slots), 0).astype(F32)).astype(F32).astype(BF16)
    closing_ref[...] = closing
    closed = nn(closing, got).astype(BF16)
    locals_ = jnp.broadcast_to(local, (HOME_ROWS, slots)).astype(BF16)
    local_ref[...] = nt(closing, locals_)
    local_lanes = nt(locals_, closing)[:1, :]
    per_map = nt(down_ref[...], closed)
    rank = per_map.shape[0] // 16
    total = jnp.zeros((rank, HOME_ROWS), F32)
    for n in range(16):
        total = total + jnp.where(local_lanes == n + 1.0, per_map[n * rank : (n + 1) * rank, :], 0.0)
    total = total.astype(BF16)
    for h in range(base_ref.shape[0]):
        parts_ref[h, :, : base_ref.shape[2]] = base_ref[h]
        parts_ref[h, :, base_ref.shape[2] :] = total
    any_pair = jnp.max(jnp.max(flags, axis=1, keepdims=True), axis=0, keepdims=True)
    served = jnp.sum(filled, axis=0, keepdims=True)
    over = jnp.maximum(any_pair, (served > HOME_ROWS).astype(F32))
    over_ref[...] = jnp.broadcast_to(over, over_ref.shape)


def home_up_kernel(parts_ref, up_ref, closing_ref, local_ref, over_ref, back_ref):
    heads, rank, wide = parts_ref.shape
    width = wide - HOME_ROWS
    slots = closing_ref.shape[1]
    total = parts_ref[0, :, width:].astype(F32)
    for h in range(1, heads):
        total = total + parts_ref[h, :, width:].astype(F32)
    ranked = jnp.concatenate([total, total], axis=0).T
    local = local_ref[...]
    stored = up_ref.shape[0] // rank
    half = iota((HOME_ROWS, 128), 1) // rank
    spread = jnp.concatenate(
        [jnp.where(local == (half + 2 * pair + 1).astype(F32), ranked, 0.0).astype(BF16) for pair in range(stored // 2)],
        axis=1,
    )
    grown = nn(spread, up_ref[...]).astype(BF16)
    opened = closing_ref[...].astype(F32).T.astype(BF16)
    back = nn(opened, grown)
    row = iota((slots, width), 0)
    back_ref[...] = jnp.where(row % BLOCK == BLOCK - 1, over_ref[:1, :1], back).astype(BF16)


def tail_kernel(back_ref, parts_ref, target_ref, out_ref, base_ref, over_ref):
    heads, rows, wide = parts_ref.shape
    slots, width = back_ref.shape
    base = parts_ref[0, :, :width].astype(F32)
    for h in range(1, heads):
        base = base + parts_ref[h, :, :width].astype(F32)
    base_ref[...] = base
    target = column(target_ref[...].astype(F32))
    picked = (iota((rows, slots), 1).astype(F32) == target).astype(F32).astype(BF16)
    back = back_ref[...]
    out_ref[...] = (base + nn(picked, back)).astype(BF16)
    peers = slots // BLOCK
    is_header = (iota((peers, slots), 1) == iota((peers, slots), 0) * BLOCK + BLOCK - 1).astype(F32).astype(BF16)
    over_ref[0, 0] = jnp.max(nn(is_header, back[:, :128]))


def call(body, outs, args, scratch=(), hbm=(), smem_out=(), flops=0):
    vmem = pl.BlockSpec(memory_space=pltpu.VMEM)
    return pl.pallas_call(
        body,
        out_shape=[jax.ShapeDtypeStruct(shape, kind) for shape, kind in outs],
        in_specs=[pl.BlockSpec(memory_space=pl.ANY) if i in hbm else vmem for i in range(len(args))],
        out_specs=[pl.BlockSpec(memory_space=pltpu.SMEM) if i in smem_out else vmem for i in range(len(outs))],
        scratch_shapes=list(scratch),
        cost_estimate=pl.CostEstimate(flops=flops, transcendentals=0, bytes_accessed=1 << 20),
    )(*args)


def from_everyone(shard, axis):
    count = lax.axis_size(axis)
    return lax.all_to_all(
        jnp.broadcast_to(shard[None], (count, *shard.shape)), axis, 0, 0, tiled=True
    )


def joined_along(blocks, dim):
    blocks = jnp.moveaxis(blocks, 0, dim)
    dims = blocks.shape
    return blocks.reshape(*dims[:dim], dims[dim] * dims[dim + 1], *dims[dim + 2 :])


def collect(shard, axis, dim):
    blocks = from_everyone(shard, axis)
    return joined_along(blocks, dim)


def exchange(blocks, axis):
    return lax.all_to_all(blocks, axis, split_axis=0, concat_axis=0, tiled=True)


def grown_by_moving_maps(
    attention, sequence_adapter_entry, batch_adapters, adapter_down_weight, adapter_up_weight
):
    rows = attention.shape[0]
    my_index = lax.axis_index("batch")
    peers = lax.axis_size("batch")
    count_each_shard = adapter_down_weight.shape[0]
    adapter_rank_width = adapter_down_weight.shape[2]
    output_width = adapter_up_weight.shape[2]
    need = batch_adapters.shape[1]
    own_list = batch_adapters[0]
    slot_match = sequence_adapter_entry[:, None] == jnp.arange(need, dtype=jnp.int32)[None, :]
    lists = collect(batch_adapters, "batch", 0)
    slot_cap = 2 * need // peers
    mine = (lists // count_each_shard == my_index).astype(jnp.int32)
    before = jnp.cumsum(mine, axis=1) - mine
    slot_range = jnp.arange(slot_cap, dtype=jnp.int32)
    select = (mine[:, None, :] == 1) & (before[:, None, :] == slot_range[None, :, None])
    shard_local_numbers = jnp.sum(
        jnp.where(select, (lists % count_each_shard)[:, None, :], 0), axis=-1
    )
    filled = jnp.any(select, axis=-1)
    stored_range = jnp.arange(count_each_shard, dtype=jnp.int32)
    one_hot = (
        (shard_local_numbers[:, :, None] == stored_range[None, None, :]) & filled[:, :, None]
    ).astype(jnp.bfloat16)
    send_shrink = jnp.einsum(
        "bcn,nkr->bckr", one_hot, adapter_down_weight, preferred_element_type=jnp.float32
    ).astype(jnp.bfloat16)
    send_expand = jnp.einsum(
        "bcn,nrw->bcrw", one_hot, adapter_up_weight, preferred_element_type=jnp.float32
    ).astype(jnp.bfloat16)
    got_shrink, got_expand = exchange(send_shrink, "batch"), exchange(send_expand, "batch")
    my_home = own_list // count_each_shard
    order_range = jnp.arange(need, dtype=jnp.int32)
    same_home = (my_home[:, None] == my_home[None, :]) & (
        order_range[None, :] < order_range[:, None]
    )
    arrival = my_home * slot_cap + jnp.sum(same_home, axis=1)
    seq_arrival = jnp.sum(jnp.where(slot_match, arrival[None, :], 0), axis=1)
    total_slots = peers * slot_cap
    picked = seq_arrival[:, None] == jnp.arange(total_slots, dtype=jnp.int32)[None, :]
    flat_shrink = got_shrink.reshape(total_slots, got_shrink.shape[2], adapter_rank_width)
    per_slot = jnp.einsum("sk,nkr->snr", attention, flat_shrink, preferred_element_type=jnp.float32)
    shrink_part = jnp.sum(per_slot * picked.astype(jnp.float32)[:, :, None], axis=1)
    ranked = lax.psum(shrink_part, "head").astype(jnp.bfloat16)
    spread = (ranked[:, None, :] * picked.astype(jnp.bfloat16)[:, :, None]).reshape(
        rows, total_slots * adapter_rank_width
    )
    return jnp.dot(
        spread,
        got_expand.reshape(total_slots * adapter_rank_width, output_width),
        preferred_element_type=jnp.float32,
    )


def per_device(
    queries,
    key_page_cache,
    value_page_cache,
    shard_page_index,
    sequence_page_count,
    last_page_tokens,
    sequence_adapter_entry,
    batch_adapters,
    output_projection_weight,
    adapter_down_weight,
    adapter_up_weight,
):
    rows, width = queries.shape
    peers = lax.axis_size("batch")
    heads = lax.axis_size("head")
    stored, _, rank = adapter_down_weight.shape
    output_width = adapter_up_weight.shape[2]
    pages = key_page_cache.shape[0]
    tokens = pages * PAGE
    slots = peers * BLOCK
    query_rows = rows * (HQ // KVH)

    send, attention, target = call(
        functools.partial(source_kernel, stored=stored, peers=peers),
        [((slots, width), BF16), ((rows, width), BF16), ((1, rows), I32)],
        [
            shard_page_index,
            sequence_page_count,
            last_page_tokens.reshape(1, rows),
            sequence_adapter_entry.reshape(1, rows),
            batch_adapters,
            queries,
            key_page_cache.reshape(tokens, HD),
            value_page_cache.reshape(tokens, HD),
        ],
        scratch=[
            pltpu.VMEM((tokens, HD), BF16),
            pltpu.VMEM((tokens, HD), BF16),
            pltpu.VMEM((query_rows, tokens), F32),
            pltpu.VMEM((tokens // 128, 128), F32),
            pltpu.SemaphoreType.DMA((2,)),
        ],
        hbm=(6, 7),
        flops=4 * query_rows * tokens * HD,
    )
    got = exchange(send.reshape(peers, BLOCK, width), "batch").reshape(slots, width)

    base = pl.pallas_call(
        base_kernel,
        grid=(heads,),
        out_shape=jax.ShapeDtypeStruct((heads, rows, output_width), BF16),
        in_specs=[
            pl.BlockSpec((rows, width), lambda h: (0, 0)),
            pl.BlockSpec((width, output_width), lambda h: (0, h)),
        ],
        out_specs=pl.BlockSpec((1, rows, output_width), lambda h: (h, 0, 0)),
        cost_estimate=pl.CostEstimate(
            flops=2 * rows * width * heads * output_width, transcendentals=0, bytes_accessed=5 << 20
        ),
    )(attention, output_projection_weight)

    wide = output_width + HOME_ROWS
    parts, closing, local, over = call(
        home_down_kernel,
        [((heads, rank, wide), BF16), ((HOME_ROWS, slots), BF16), ((HOME_ROWS, HOME_ROWS), F32), ((8, 128), F32)],
        [got, jnp.swapaxes(adapter_down_weight, 1, 2).reshape(stored * rank, width), base],
        flops=2 * HOME_ROWS * width * stored * rank,
    )
    parts = exchange(parts, "head")
    (back,) = call(
        home_up_kernel,
        [((slots, output_width), BF16)],
        [parts, adapter_up_weight.reshape(stored * rank, output_width), closing, local, over],
        flops=2 * HOME_ROWS * output_width * stored * rank,
    )
    back = exchange(back.reshape(peers, BLOCK, output_width), "batch").reshape(slots, output_width)
    out, base, over = call(
        tail_kernel,
        [((rows, output_width), BF16), ((rows, output_width), F32), ((1, 1), F32)],
        [back, parts, target],
        smem_out=(2,),
        flops=2 * rows * slots * output_width,
    )

    def moving():
        grown = grown_by_moving_maps(
            attention, sequence_adapter_entry, batch_adapters, adapter_down_weight, adapter_up_weight
        )
        return (base + grown).astype(BF16)

    return lax.cond(over[0, 0] > 0.0, moving, lambda: out)


def solution(mesh):
    in_specs = (
        P("batch", "head"),
        P("batch", None, "head"),
        P("batch", None, "head"),
        P("batch", None),
        P("batch", None),
        P("batch"),
        P("batch"),
        P("batch", None),
        P("head", None),
        P("batch", "head", None),
        P("batch", None, "head"),
    )
    out_specs = P("batch", "head")
    return jax.shard_map(
        per_device, mesh=mesh, in_specs=in_specs, out_specs=out_specs, check_vma=False
    )
```

```python
import functools

import jax
import jax.numpy as jnp
from jax import lax
from jax.experimental import pallas as pl
from jax.experimental.pallas import tpu as pltpu
from jax.sharding import PartitionSpec as P

HQ = 32
KVH = 8
HD = 128
PAGE = 16
BLOCK = 16
HOME_ROWS = 128
CHUNK = 512
F32, BF16, I32 = jnp.float32, jnp.bfloat16, jnp.int32


def iota(shape, dim):
    return lax.broadcasted_iota(I32, shape, dim)


def nn(a, b):
    return lax.dot_general(a, b, (((1,), (0,)), ((), ())), preferred_element_type=F32)


def nt(a, b):
    return lax.dot_general(a, b, (((1,), (1,)), ((), ())), preferred_element_type=F32)


def column(row):
    n = row.shape[1]
    return jnp.sum(jnp.where(iota((n, n), 0) == iota((n, n), 1), row, 0.0), axis=1, keepdims=True)


def source_kernel(
    index_ref,
    count_ref,
    last_ref,
    entry_ref,
    list_ref,
    q_ref,
    keys_hbm,
    values_hbm,
    send_ref,
    attention_ref,
    target_ref,
    keys_ref,
    values_ref,
    scores_ref,
    owner_ref,
    sems,
    *,
    stored,
    peers,
):
    rows = q_ref.shape[0]
    pages = index_ref.shape[1]
    tokens = pages * PAGE
    groups = HQ // KVH
    steps = tokens // CHUNK
    copy_keys = pltpu.make_async_copy(keys_hbm, keys_ref, sems.at[0])
    copy_values = pltpu.make_async_copy(values_hbm, values_ref, sems.at[1])
    copy_keys.start()
    copy_values.start()

    count = count_ref[...].astype(F32)
    end = jnp.sum(jnp.where(iota((rows, rows), 1) <= iota((rows, rows), 0), count, 0.0), axis=1, keepdims=True)
    last = column(last_ref[...].astype(F32))
    position = iota((rows, pages), 1).astype(F32)
    owner = jnp.sum((end <= position).astype(F32), axis=0, keepdims=True)
    limit = PAGE - jnp.sum(jnp.where(position == end - 1.0, PAGE - last, 0.0), axis=0, keepdims=True)
    index = index_ref[...]
    per_row = 128 // PAGE
    high = iota((tokens // 128, pages), 0) == index // per_row
    low = (iota((128, pages), 0) // PAGE == index % per_row).astype(F32).astype(BF16)
    owner = nt(jnp.where(high, owner, 0.0).astype(BF16), low)
    limit = nt(jnp.where(high, limit, 0.0).astype(BF16), low)
    inside = (iota((tokens // 128, 128), 1) % PAGE).astype(F32) < limit
    owner_ref[...] = jnp.where(inside, owner, -1.0)

    adapters = list_ref[...].astype(F32)
    entry = entry_ref[...].astype(F32)
    need = adapters.shape[1]
    ids_row = jnp.sum(
        jnp.where(iota((need, rows), 0).astype(F32) == entry, column(adapters), 0.0), axis=0, keepdims=True
    )
    ids_col = column(ids_row)
    home_row = ids_row.astype(I32) // stored
    home_col = ids_col.astype(I32) // stored
    local_row = ids_row.astype(I32) % stored
    same = home_col == home_row
    sub, lane = iota((rows, rows), 0), iota((rows, rows), 1)
    place_row = jnp.sum((same & (sub < lane)).astype(F32), axis=0, keepdims=True).astype(I32)
    place_col = jnp.sum((same & (lane < sub)).astype(F32), axis=1, keepdims=True).astype(I32)
    target = jnp.where(place_row < BLOCK - 1, home_row * BLOCK + place_row, -1)
    target_ref[...] = target
    over = jnp.max(place_row.astype(F32), axis=1, keepdims=True) >= BLOCK - 1
    width = q_ref.shape[1]
    heads_of = jnp.where(iota((peers, rows), 0) == home_row, local_row + 1, 0).astype(F32).astype(BF16)
    spread = (iota((rows, width), 1) % BLOCK == place_col).astype(F32).astype(BF16)
    header = nn(heads_of, spread)
    header = jnp.where(iota((peers, width), 1) % BLOCK == BLOCK - 1, over.astype(F32), header).astype(BF16)

    q = jnp.concatenate([q_ref[:, g * HD : (g + 1) * HD] for g in range(groups)], axis=0)
    own = (iota((groups * rows, 128), 0) % rows).astype(F32)
    copy_keys.wait()
    top = jnp.full((groups * rows, 128), -1e30, F32)
    for step in range(steps):
        block = nt(q, keys_ref[step * CHUNK : (step + 1) * CHUNK, :])
        for part in range(CHUNK // 128):
            at = step * (CHUNK // 128) + part
            kept = jnp.where(owner_ref[at : at + 1, :] == own, block[:, part * 128 : (part + 1) * 128], -1e30)
            scores_ref[:, at * 128 : (at + 1) * 128] = kept
            top = jnp.maximum(top, kept)
    factor = HD**-0.5 * 1.4426950408889634
    top = jnp.max(top, axis=1, keepdims=True)
    copy_values.wait()
    total = jnp.zeros((groups * rows, 128), F32)
    mixed = jnp.zeros((groups * rows, HD), F32)
    for step in range(steps):
        powers = jnp.exp2((scores_ref[:, step * CHUNK : (step + 1) * CHUNK] - top) * factor)
        for part in range(CHUNK // 128):
            total = total + powers[:, part * 128 : (part + 1) * 128]
        mixed = mixed + nn(powers.astype(BF16), values_ref[step * CHUNK : (step + 1) * CHUNK, :])
    mixed = (mixed / jnp.sum(total, axis=1, keepdims=True)).astype(BF16)
    attention = jnp.concatenate([mixed[g * rows : (g + 1) * rows] for g in range(groups)], axis=1)
    attention_ref[...] = attention

    slots = peers * BLOCK
    picked = jnp.concatenate(
        [
            (iota((slots, rows), 0) == target).astype(F32),
            (iota((slots, peers), 0) == iota((slots, peers), 1) * BLOCK + BLOCK - 1).astype(F32),
        ],
        axis=1,
    ).astype(BF16)
    send_ref[...] = nn(picked, jnp.concatenate([attention, header], axis=0)).astype(BF16)


def base_kernel(attention_ref, weight_ref, out_ref):
    out_ref[0] = nn(attention_ref[...], weight_ref[...]).astype(BF16)


def home_down_kernel(got_ref, down_ref, base_ref, parts_ref, closing_ref, local_ref, over_ref):
    slots, width = got_ref.shape
    peers = slots // BLOCK
    got = got_ref[...]
    is_header = (iota((peers, slots), 1) == iota((peers, slots), 0) * BLOCK + BLOCK - 1).astype(F32).astype(BF16)
    header = nn(is_header, got)[:, :slots]
    lane = iota((peers, slots), 1)
    sub = iota((peers, slots), 0)
    flags = jnp.where(lane % BLOCK == BLOCK - 1, header, 0.0)
    ids = jnp.where(lane % BLOCK == BLOCK - 1, 0.0, header)
    ids_first = jnp.where(lane < BLOCK, ids, 0.0)
    filled = jnp.sum((ids_first > 0.0).astype(F32), axis=1, keepdims=True)
    before = jnp.sum(jnp.where(sub < lane // BLOCK, filled, 0.0), axis=0, keepdims=True)
    here = jnp.sum(jnp.where(sub == lane // BLOCK, filled, 0.0), axis=0, keepdims=True)
    local = jnp.sum(jnp.where(sub == lane // BLOCK, ids, 0.0), axis=0, keepdims=True)
    within = (iota((1, slots), 1) % BLOCK).astype(F32)
    at = jnp.where(within < here, before + within, -1.0)
    closing = (at == iota((HOME_ROWS, slots), 0).astype(F32)).astype(F32).astype(BF16)
    closing_ref[...] = closing
    closed = nn(closing, got).astype(BF16)
    locals_ = jnp.broadcast_to(local, (HOME_ROWS, slots)).astype(BF16)
    local_ref[...] = nt(closing, locals_)
    local_lanes = nt(locals_, closing)[:1, :]
    per_map = nt(down_ref[...], closed)
    rank = per_map.shape[0] // 16
    total = jnp.zeros((rank, HOME_ROWS), F32)
    for n in range(16):
        total = total + jnp.where(local_lanes == n + 1.0, per_map[n * rank : (n + 1) * rank, :], 0.0)
    total = total.astype(BF16)
    for h in range(base_ref.shape[0]):
        parts_ref[h, :, : base_ref.shape[2]] = base_ref[h]
        parts_ref[h, :, base_ref.shape[2] :] = total
    any_pair = jnp.max(jnp.max(flags, axis=1, keepdims=True), axis=0, keepdims=True)
    served = jnp.sum(filled, axis=0, keepdims=True)
    over = jnp.maximum(any_pair, (served > HOME_ROWS).astype(F32))
    over_ref[...] = jnp.broadcast_to(over, over_ref.shape)


def home_up_kernel(parts_ref, up_ref, closing_ref, local_ref, over_ref, back_ref):
    heads, rank, wide = parts_ref.shape
    width = wide - HOME_ROWS
    slots = closing_ref.shape[1]
    total = parts_ref[0, :, width:].astype(F32)
    for h in range(1, heads):
        total = total + parts_ref[h, :, width:].astype(F32)
    ranked = jnp.concatenate([total, total], axis=0).T
    local = local_ref[...]
    stored = up_ref.shape[0] // rank
    half = iota((HOME_ROWS, 128), 1) // rank
    spread = jnp.concatenate(
        [jnp.where(local == (half + 2 * pair + 1).astype(F32), ranked, 0.0).astype(BF16) for pair in range(stored // 2)],
        axis=1,
    )
    grown = nn(spread, up_ref[...]).astype(BF16)
    opened = closing_ref[...].astype(F32).T.astype(BF16)
    back = nn(opened, grown)
    row = iota((slots, width), 0)
    back_ref[...] = jnp.where(row % BLOCK == BLOCK - 1, over_ref[:1, :1], back).astype(BF16)


def tail_kernel(back_ref, parts_ref, target_ref, out_ref, base_ref, over_ref):
    heads, rows, wide = parts_ref.shape
    slots, width = back_ref.shape
    base = parts_ref[0, :, :width].astype(F32)
    for h in range(1, heads):
        base = base + parts_ref[h, :, :width].astype(F32)
    base_ref[...] = base
    target = column(target_ref[...].astype(F32))
    picked = (iota((rows, slots), 1).astype(F32) == target).astype(F32).astype(BF16)
    back = back_ref[...]
    out_ref[...] = (base + nn(picked, back)).astype(BF16)
    peers = slots // BLOCK
    is_header = (iota((peers, slots), 1) == iota((peers, slots), 0) * BLOCK + BLOCK - 1).astype(F32).astype(BF16)
    over_ref[0, 0] = (jnp.max(nn(is_header, back[:, :128])) > 0.0).astype(I32)


def call(body, outs, args, scratch=(), hbm=(), smem_out=(), flops=0, mib=8):
    vmem = pl.BlockSpec(memory_space=pltpu.VMEM)
    return pl.pallas_call(
        body,
        out_shape=[jax.ShapeDtypeStruct(shape, kind) for shape, kind in outs],
        in_specs=[pl.BlockSpec(memory_space=pltpu.HBM) if i in hbm else vmem for i in range(len(args))],
        out_specs=[pl.BlockSpec(memory_space=pltpu.SMEM) if i in smem_out else vmem for i in range(len(outs))],
        scratch_shapes=list(scratch),
        cost_estimate=pl.CostEstimate(flops=flops, transcendentals=0, bytes_accessed=1 << 20),
        compiler_params=pltpu.CompilerParams(vmem_limit_bytes=mib << 20),
    )(*args)


def from_everyone(shard, axis):
    count = lax.axis_size(axis)
    return lax.all_to_all(
        jnp.broadcast_to(shard[None], (count, *shard.shape)), axis, 0, 0, tiled=True
    )


def joined_along(blocks, dim):
    blocks = jnp.moveaxis(blocks, 0, dim)
    dims = blocks.shape
    return blocks.reshape(*dims[:dim], dims[dim] * dims[dim + 1], *dims[dim + 2 :])


def collect(shard, axis, dim):
    blocks = from_everyone(shard, axis)
    return joined_along(blocks, dim)


def exchange(blocks, axis):
    return lax.all_to_all(blocks, axis, split_axis=0, concat_axis=0, tiled=True)


def grown_by_moving_maps(
    attention, sequence_adapter_entry, batch_adapters, adapter_down_weight, adapter_up_weight
):
    rows = attention.shape[0]
    my_index = lax.axis_index("batch")
    peers = lax.axis_size("batch")
    count_each_shard = adapter_down_weight.shape[0]
    adapter_rank_width = adapter_down_weight.shape[2]
    output_width = adapter_up_weight.shape[2]
    need = batch_adapters.shape[1]
    own_list = batch_adapters[0]
    slot_match = sequence_adapter_entry[:, None] == jnp.arange(need, dtype=jnp.int32)[None, :]
    lists = collect(batch_adapters, "batch", 0)
    slot_cap = 2 * need // peers
    mine = (lists // count_each_shard == my_index).astype(jnp.int32)
    before = jnp.cumsum(mine, axis=1) - mine
    slot_range = jnp.arange(slot_cap, dtype=jnp.int32)
    select = (mine[:, None, :] == 1) & (before[:, None, :] == slot_range[None, :, None])
    shard_local_numbers = jnp.sum(
        jnp.where(select, (lists % count_each_shard)[:, None, :], 0), axis=-1
    )
    filled = jnp.any(select, axis=-1)
    stored_range = jnp.arange(count_each_shard, dtype=jnp.int32)
    one_hot = (
        (shard_local_numbers[:, :, None] == stored_range[None, None, :]) & filled[:, :, None]
    ).astype(jnp.bfloat16)
    send_shrink = jnp.einsum(
        "bcn,nkr->bckr", one_hot, adapter_down_weight, preferred_element_type=jnp.float32
    ).astype(jnp.bfloat16)
    send_expand = jnp.einsum(
        "bcn,nrw->bcrw", one_hot, adapter_up_weight, preferred_element_type=jnp.float32
    ).astype(jnp.bfloat16)
    got_shrink, got_expand = exchange(send_shrink, "batch"), exchange(send_expand, "batch")
    my_home = own_list // count_each_shard
    order_range = jnp.arange(need, dtype=jnp.int32)
    same_home = (my_home[:, None] == my_home[None, :]) & (
        order_range[None, :] < order_range[:, None]
    )
    arrival = my_home * slot_cap + jnp.sum(same_home, axis=1)
    seq_arrival = jnp.sum(jnp.where(slot_match, arrival[None, :], 0), axis=1)
    total_slots = peers * slot_cap
    picked = seq_arrival[:, None] == jnp.arange(total_slots, dtype=jnp.int32)[None, :]
    flat_shrink = got_shrink.reshape(total_slots, got_shrink.shape[2], adapter_rank_width)
    per_slot = jnp.einsum("sk,nkr->snr", attention, flat_shrink, preferred_element_type=jnp.float32)
    shrink_part = jnp.sum(per_slot * picked.astype(jnp.float32)[:, :, None], axis=1)
    ranked = lax.psum(shrink_part, "head").astype(jnp.bfloat16)
    spread = (ranked[:, None, :] * picked.astype(jnp.bfloat16)[:, :, None]).reshape(
        rows, total_slots * adapter_rank_width
    )
    return jnp.dot(
        spread,
        got_expand.reshape(total_slots * adapter_rank_width, output_width),
        preferred_element_type=jnp.float32,
    )


def per_device(
    queries,
    key_page_cache,
    value_page_cache,
    shard_page_index,
    sequence_page_count,
    last_page_tokens,
    sequence_adapter_entry,
    batch_adapters,
    output_projection_weight,
    adapter_down_weight,
    adapter_up_weight,
):
    rows, width = queries.shape
    peers = lax.axis_size("batch")
    heads = lax.axis_size("head")
    stored, _, rank = adapter_down_weight.shape
    output_width = adapter_up_weight.shape[2]
    pages = key_page_cache.shape[0]
    tokens = pages * PAGE
    slots = peers * BLOCK
    query_rows = rows * (HQ // KVH)

    send, attention, target = call(
        functools.partial(source_kernel, stored=stored, peers=peers),
        [((slots, width), BF16), ((rows, width), BF16), ((1, rows), I32)],
        [
            shard_page_index,
            sequence_page_count,
            last_page_tokens.reshape(1, rows),
            sequence_adapter_entry.reshape(1, rows),
            batch_adapters,
            queries,
            key_page_cache.reshape(tokens, HD),
            value_page_cache.reshape(tokens, HD),
        ],
        scratch=[
            pltpu.VMEM((tokens, HD), BF16),
            pltpu.VMEM((tokens, HD), BF16),
            pltpu.VMEM((query_rows, tokens), F32),
            pltpu.VMEM((tokens // 128, 128), F32),
            pltpu.SemaphoreType.DMA((2,)),
        ],
        hbm=(6, 7),
        mib=60,
        flops=4 * query_rows * tokens * HD,
    )
    got = exchange(send.reshape(peers, BLOCK, width), "batch").reshape(slots, width)

    base = pl.pallas_call(
        base_kernel,
        grid=(heads,),
        out_shape=jax.ShapeDtypeStruct((heads, rows, output_width), BF16),
        in_specs=[
            pl.BlockSpec((rows, width), lambda h: (0, 0)),
            pl.BlockSpec((width, output_width), lambda h: (0, h)),
        ],
        out_specs=pl.BlockSpec((1, rows, output_width), lambda h: (h, 0, 0)),
        cost_estimate=pl.CostEstimate(
            flops=2 * rows * width * heads * output_width, transcendentals=0, bytes_accessed=5 << 20
        ),
        compiler_params=pltpu.CompilerParams(vmem_limit_bytes=8 << 20),
    )(attention, output_projection_weight)

    wide = output_width + HOME_ROWS
    parts, closing, local, over = call(
        home_down_kernel,
        [((heads, rank, wide), BF16), ((HOME_ROWS, slots), BF16), ((HOME_ROWS, HOME_ROWS), F32), ((8, 128), F32)],
        [got, jnp.swapaxes(adapter_down_weight, 1, 2).reshape(stored * rank, width), base],
        flops=2 * HOME_ROWS * width * stored * rank,
    )
    parts = exchange(parts, "head")
    (back,) = call(
        home_up_kernel,
        [((slots, output_width), BF16)],
        [parts, adapter_up_weight.reshape(stored * rank, output_width), closing, local, over],
        flops=2 * HOME_ROWS * output_width * stored * rank,
    )
    back = exchange(back.reshape(peers, BLOCK, output_width), "batch").reshape(slots, output_width)
    out, base, over = call(
        tail_kernel,
        [((rows, output_width), BF16), ((rows, output_width), F32), ((1, 1), I32)],
        [back, parts, target],
        smem_out=(2,),
        flops=2 * rows * slots * output_width,
    )

    def moving():
        grown = grown_by_moving_maps(
            attention, sequence_adapter_entry, batch_adapters, adapter_down_weight, adapter_up_weight
        )
        return (base + grown).astype(BF16)

    return lax.switch(over[0, 0], [lambda: out, moving])


def solution(mesh):
    in_specs = (
        P("batch", "head"),
        P("batch", None, "head"),
        P("batch", None, "head"),
        P("batch", None),
        P("batch", None),
        P("batch"),
        P("batch"),
        P("batch", None),
        P("head", None),
        P("batch", "head", None),
        P("batch", None, "head"),
    )
    out_specs = P("batch", "head")
    return jax.shard_map(
        per_device, mesh=mesh, in_specs=in_specs, out_specs=out_specs, check_vma=False
    )
```

```python
import functools

import jax
import jax.numpy as jnp
from jax import lax
from jax.experimental import pallas as pl
from jax.experimental.pallas import tpu as pltpu
from jax.sharding import PartitionSpec as P

HQ = 32
KVH = 8
HD = 128
PAGE = 16
BLOCK = 16
HOME_ROWS = 128
CHUNK = 512
PIECES = 4
F32, BF16, I32 = jnp.float32, jnp.bfloat16, jnp.int32


def iota(shape, dim):
    return lax.broadcasted_iota(I32, shape, dim)


def nn(a, b):
    return lax.dot_general(a, b, (((1,), (0,)), ((), ())), preferred_element_type=F32)


def nt(a, b):
    return lax.dot_general(a, b, (((1,), (1,)), ((), ())), preferred_element_type=F32)


def column(row):
    n = row.shape[1]
    return jnp.sum(jnp.where(iota((n, n), 0) == iota((n, n), 1), row, 0.0), axis=1, keepdims=True)


def source_kernel(
    index_hbm,
    count_hbm,
    last_hbm,
    entry_hbm,
    list_hbm,
    q_hbm,
    keys_hbm,
    values_hbm,
    send_ref,
    attention_ref,
    target_ref,
    index_ref,
    count_ref,
    last_ref,
    entry_ref,
    list_ref,
    q_ref,
    keys_ref,
    values_ref,
    scores_ref,
    owner_ref,
    sems,
    *,
    stored,
    peers,
):
    rows = q_ref.shape[0]
    pages = index_ref.shape[1]
    tokens = pages * PAGE
    groups = HQ // KVH
    steps = tokens // CHUNK
    piece = tokens // PIECES
    small = [
        pltpu.make_async_copy(source, target, sems.at[n])
        for n, (source, target) in enumerate(
            [
                (count_hbm, count_ref),
                (last_hbm, last_ref),
                (index_hbm, index_ref),
                (entry_hbm, entry_ref),
                (list_hbm, list_ref),
                (q_hbm, q_ref),
            ]
        )
    ]
    copy_keys = [
        pltpu.make_async_copy(
            keys_hbm.at[pl.ds(n * piece, piece)], keys_ref.at[pl.ds(n * piece, piece)], sems.at[6 + n]
        )
        for n in range(PIECES)
    ]
    copy_values = pltpu.make_async_copy(values_hbm, values_ref, sems.at[6 + PIECES])
    for copy in small:
        copy.start()
    for copy in copy_keys:
        copy.start()
    copy_values.start()
    for copy in small:
        copy.wait()

    count = count_ref[...].astype(F32)
    end = jnp.sum(jnp.where(iota((rows, rows), 1) <= iota((rows, rows), 0), count, 0.0), axis=1, keepdims=True)
    last = column(last_ref[...].astype(F32))
    position = iota((rows, pages), 1).astype(F32)
    owner = jnp.sum((end <= position).astype(F32), axis=0, keepdims=True)
    limit = PAGE - jnp.sum(jnp.where(position == end - 1.0, PAGE - last, 0.0), axis=0, keepdims=True)
    index = index_ref[...]
    per_row = 128 // PAGE
    high = iota((tokens // 128, pages), 0) == index // per_row
    low = (iota((128, pages), 0) // PAGE == index % per_row).astype(F32).astype(BF16)
    owner = nt(jnp.where(high, owner, 0.0).astype(BF16), low)
    limit = nt(jnp.where(high, limit, 0.0).astype(BF16), low)
    inside = (iota((tokens // 128, 128), 1) % PAGE).astype(F32) < limit
    owner_ref[...] = jnp.where(inside, owner, -1.0)

    adapters = list_ref[...].astype(F32)
    entry = entry_ref[...].astype(F32)
    need = adapters.shape[1]
    ids_row = jnp.sum(
        jnp.where(iota((need, rows), 0).astype(F32) == entry, column(adapters), 0.0), axis=0, keepdims=True
    )
    ids_col = column(ids_row)
    home_row = ids_row.astype(I32) // stored
    home_col = ids_col.astype(I32) // stored
    local_row = ids_row.astype(I32) % stored
    same = home_col == home_row
    sub, lane = iota((rows, rows), 0), iota((rows, rows), 1)
    place_row = jnp.sum((same & (sub < lane)).astype(F32), axis=0, keepdims=True).astype(I32)
    place_col = jnp.sum((same & (lane < sub)).astype(F32), axis=1, keepdims=True).astype(I32)
    target = jnp.where(place_row < BLOCK - 1, home_row * BLOCK + place_row, -1)
    target_ref[...] = target
    over = jnp.max(place_row.astype(F32), axis=1, keepdims=True) >= BLOCK - 1
    width = q_ref.shape[1]
    heads_of = jnp.where(iota((peers, rows), 0) == home_row, local_row + 1, 0).astype(F32).astype(BF16)
    spread = (iota((rows, width), 1) % BLOCK == place_col).astype(F32).astype(BF16)
    header = nn(heads_of, spread)
    header = jnp.where(iota((peers, width), 1) % BLOCK == BLOCK - 1, over.astype(F32), header).astype(BF16)

    q = jnp.concatenate([q_ref[:, g * HD : (g + 1) * HD] for g in range(groups)], axis=0)
    own = (iota((groups * rows, 128), 0) % rows).astype(F32)
    top = jnp.full((groups * rows, 128), -1e30, F32)
    for step in range(steps):
        if step * CHUNK % piece == 0:
            copy_keys[step * CHUNK // piece].wait()
        block = nt(q, keys_ref[step * CHUNK : (step + 1) * CHUNK, :])
        for part in range(CHUNK // 128):
            at = step * (CHUNK // 128) + part
            kept = jnp.where(owner_ref[at : at + 1, :] == own, block[:, part * 128 : (part + 1) * 128], -1e30)
            scores_ref[:, at * 128 : (at + 1) * 128] = kept
            top = jnp.maximum(top, kept)
    factor = HD**-0.5 * 1.4426950408889634
    top = jnp.max(top, axis=1, keepdims=True)
    copy_values.wait()
    total = jnp.zeros((groups * rows, 128), F32)
    mixed = jnp.zeros((groups * rows, HD), F32)
    for step in range(steps):
        powers = jnp.exp2((scores_ref[:, step * CHUNK : (step + 1) * CHUNK] - top) * factor)
        for part in range(CHUNK // 128):
            total = total + powers[:, part * 128 : (part + 1) * 128]
        mixed = mixed + nn(powers.astype(BF16), values_ref[step * CHUNK : (step + 1) * CHUNK, :])
    mixed = (mixed / jnp.sum(total, axis=1, keepdims=True)).astype(BF16)
    attention = jnp.concatenate([mixed[g * rows : (g + 1) * rows] for g in range(groups)], axis=1)
    attention_ref[...] = attention

    slots = peers * BLOCK
    picked = jnp.concatenate(
        [
            (iota((slots, rows), 0) == target).astype(F32),
            (iota((slots, peers), 0) == iota((slots, peers), 1) * BLOCK + BLOCK - 1).astype(F32),
        ],
        axis=1,
    ).astype(BF16)
    send_ref[...] = nn(picked, jnp.concatenate([attention, header], axis=0)).astype(BF16)


def base_kernel(core_ref, attention_ref, weight_ref, keep_ref, give_ref):
    half = keep_ref.shape[1]
    core = core_ref[0, 0]
    product = nn(attention_ref[...], weight_ref[...])
    first, second = product[:half], product[half:]
    keep_ref[0] = jnp.where(core == 0, first, second).astype(BF16)
    give_ref[0] = jnp.where(core == 0, second, first).astype(BF16)


def home_down_kernel(got_ref, down_ref, keep_ref, sibling_ref, parts_ref, closing_ref, local_ref, over_ref):
    slots, width = got_ref.shape
    peers = slots // BLOCK
    got = got_ref[...]
    is_header = (iota((peers, slots), 1) == iota((peers, slots), 0) * BLOCK + BLOCK - 1).astype(F32).astype(BF16)
    header = nn(is_header, got)[:, :slots]
    lane = iota((peers, slots), 1)
    sub = iota((peers, slots), 0)
    flags = jnp.where(lane % BLOCK == BLOCK - 1, header, 0.0)
    ids = jnp.where(lane % BLOCK == BLOCK - 1, 0.0, header)
    ids_first = jnp.where(lane < BLOCK, ids, 0.0)
    filled = jnp.sum((ids_first > 0.0).astype(F32), axis=1, keepdims=True)
    before = jnp.sum(jnp.where(sub < lane // BLOCK, filled, 0.0), axis=0, keepdims=True)
    here = jnp.sum(jnp.where(sub == lane // BLOCK, filled, 0.0), axis=0, keepdims=True)
    local = jnp.sum(jnp.where(sub == lane // BLOCK, ids, 0.0), axis=0, keepdims=True)
    within = (iota((1, slots), 1) % BLOCK).astype(F32)
    at = jnp.where(within < here, before + within, -1.0)
    closing = (at == iota((HOME_ROWS, slots), 0).astype(F32)).astype(F32).astype(BF16)
    closing_ref[...] = closing
    closed = nn(closing, got).astype(BF16)
    locals_ = jnp.broadcast_to(local, (HOME_ROWS, slots)).astype(BF16)
    local_ref[...] = nt(closing, locals_)
    local_lanes = nt(locals_, closing)[:1, :]
    per_map = nt(down_ref[...], closed)
    rank = per_map.shape[0] // 16
    total = jnp.zeros((rank, HOME_ROWS), F32)
    for n in range(16):
        total = total + jnp.where(local_lanes == n + 1.0, per_map[n * rank : (n + 1) * rank, :], 0.0)
    total = total.astype(BF16)
    heads, half, output_width = keep_ref.shape
    total = jnp.concatenate([total[:half], total[half:]], axis=1)
    for h in range(heads):
        both = keep_ref[h].astype(F32) + sibling_ref[h].astype(F32)
        parts_ref[h, :, :output_width] = both.astype(BF16)
        parts_ref[h, :, output_width:] = total
    any_pair = jnp.max(jnp.max(flags, axis=1, keepdims=True), axis=0, keepdims=True)
    served = jnp.sum(filled, axis=0, keepdims=True)
    over = jnp.maximum(any_pair, (served > HOME_ROWS).astype(F32))
    over_ref[...] = jnp.broadcast_to(over, over_ref.shape)


def home_up_kernel(parts_ref, up_ref, closing_ref, local_ref, over_ref, back_ref):
    heads, half, wide = parts_ref.shape
    rank = 2 * half
    width = wide - 2 * HOME_ROWS
    slots = closing_ref.shape[1]
    total = parts_ref[0, :, width:].astype(F32)
    for h in range(1, heads):
        total = total + parts_ref[h, :, width:].astype(F32)
    total = jnp.concatenate([total[:, :HOME_ROWS], total[:, HOME_ROWS:]], axis=0)
    ranked = jnp.concatenate([total, total], axis=0).T
    local = local_ref[...]
    stored = up_ref.shape[0] // rank
    side = iota((HOME_ROWS, 128), 1) // rank
    spread = jnp.concatenate(
        [jnp.where(local == (side + 2 * pair + 1).astype(F32), ranked, 0.0).astype(BF16) for pair in range(stored // 2)],
        axis=1,
    )
    grown = nn(spread, up_ref[...]).astype(BF16)
    opened = closing_ref[...].astype(F32).T.astype(BF16)
    back = nn(opened, grown)
    row = iota((slots, width), 0)
    back_ref[...] = jnp.where(row % BLOCK == BLOCK - 1, over_ref[:1, :1], back).astype(BF16)


def tail_kernel(back_ref, parts_ref, target_ref, out_ref, base_ref, over_ref):
    heads, half, wide = parts_ref.shape
    rows = 2 * half
    slots, width = back_ref.shape
    base = [parts_ref[core, :, :width].astype(F32) for core in range(2)]
    for h in range(2, heads):
        base[h % 2] = base[h % 2] + parts_ref[h, :, :width].astype(F32)
    base = jnp.concatenate(base, axis=0)
    base_ref[...] = base
    target = column(target_ref[...].astype(F32))
    picked = (iota((rows, slots), 1).astype(F32) == target).astype(F32).astype(BF16)
    back = back_ref[...]
    out_ref[...] = (base + nn(picked, back)).astype(BF16)
    peers = slots // BLOCK
    is_header = (iota((peers, slots), 1) == iota((peers, slots), 0) * BLOCK + BLOCK - 1).astype(F32).astype(BF16)
    over_ref[0, 0] = (jnp.max(nn(is_header, back[:, :128])) > 0.0).astype(I32)


def call(body, outs, args, scratch=(), hbm=(), smem_out=(), flops=0, mib=8):
    vmem = pl.BlockSpec(memory_space=pltpu.VMEM)
    return pl.pallas_call(
        body,
        out_shape=[jax.ShapeDtypeStruct(shape, kind) for shape, kind in outs],
        in_specs=[pl.BlockSpec(memory_space=pltpu.HBM) if i in hbm else vmem for i in range(len(args))],
        out_specs=[pl.BlockSpec(memory_space=pltpu.SMEM) if i in smem_out else vmem for i in range(len(outs))],
        scratch_shapes=list(scratch),
        cost_estimate=pl.CostEstimate(flops=flops, transcendentals=0, bytes_accessed=1 << 20),
        compiler_params=pltpu.CompilerParams(vmem_limit_bytes=mib << 20),
    )(*args)


def from_everyone(shard, axis):
    count = lax.axis_size(axis)
    return lax.all_to_all(
        jnp.broadcast_to(shard[None], (count, *shard.shape)), axis, 0, 0, tiled=True
    )


def joined_along(blocks, dim):
    blocks = jnp.moveaxis(blocks, 0, dim)
    dims = blocks.shape
    return blocks.reshape(*dims[:dim], dims[dim] * dims[dim + 1], *dims[dim + 2 :])


def collect(shard, axis, dim):
    blocks = from_everyone(shard, axis)
    return joined_along(blocks, dim)


def exchange(blocks, axis):
    return lax.all_to_all(blocks, axis, split_axis=0, concat_axis=0, tiled=True)


def grown_by_moving_maps(
    attention, sequence_adapter_entry, batch_adapters, adapter_down_weight, adapter_up_weight
):
    rows = attention.shape[0]
    my_index = lax.axis_index("batch")
    peers = lax.axis_size("batch")
    count_each_shard = adapter_down_weight.shape[0]
    adapter_rank_width = adapter_down_weight.shape[2]
    output_width = adapter_up_weight.shape[2]
    need = batch_adapters.shape[1]
    own_list = batch_adapters[0]
    slot_match = sequence_adapter_entry[:, None] == jnp.arange(need, dtype=jnp.int32)[None, :]
    lists = collect(batch_adapters, "batch", 0)
    slot_cap = 2 * need // peers
    mine = (lists // count_each_shard == my_index).astype(jnp.int32)
    before = jnp.cumsum(mine, axis=1) - mine
    slot_range = jnp.arange(slot_cap, dtype=jnp.int32)
    select = (mine[:, None, :] == 1) & (before[:, None, :] == slot_range[None, :, None])
    shard_local_numbers = jnp.sum(
        jnp.where(select, (lists % count_each_shard)[:, None, :], 0), axis=-1
    )
    filled = jnp.any(select, axis=-1)
    stored_range = jnp.arange(count_each_shard, dtype=jnp.int32)
    one_hot = (
        (shard_local_numbers[:, :, None] == stored_range[None, None, :]) & filled[:, :, None]
    ).astype(jnp.bfloat16)
    send_shrink = jnp.einsum(
        "bcn,nkr->bckr", one_hot, adapter_down_weight, preferred_element_type=jnp.float32
    ).astype(jnp.bfloat16)
    send_expand = jnp.einsum(
        "bcn,nrw->bcrw", one_hot, adapter_up_weight, preferred_element_type=jnp.float32
    ).astype(jnp.bfloat16)
    got_shrink, got_expand = exchange(send_shrink, "batch"), exchange(send_expand, "batch")
    my_home = own_list // count_each_shard
    order_range = jnp.arange(need, dtype=jnp.int32)
    same_home = (my_home[:, None] == my_home[None, :]) & (
        order_range[None, :] < order_range[:, None]
    )
    arrival = my_home * slot_cap + jnp.sum(same_home, axis=1)
    seq_arrival = jnp.sum(jnp.where(slot_match, arrival[None, :], 0), axis=1)
    total_slots = peers * slot_cap
    picked = seq_arrival[:, None] == jnp.arange(total_slots, dtype=jnp.int32)[None, :]
    flat_shrink = got_shrink.reshape(total_slots, got_shrink.shape[2], adapter_rank_width)
    per_slot = jnp.einsum("sk,nkr->snr", attention, flat_shrink, preferred_element_type=jnp.float32)
    shrink_part = jnp.sum(per_slot * picked.astype(jnp.float32)[:, :, None], axis=1)
    ranked = lax.psum(shrink_part, "head").astype(jnp.bfloat16)
    spread = (ranked[:, None, :] * picked.astype(jnp.bfloat16)[:, :, None]).reshape(
        rows, total_slots * adapter_rank_width
    )
    return jnp.dot(
        spread,
        got_expand.reshape(total_slots * adapter_rank_width, output_width),
        preferred_element_type=jnp.float32,
    )


def per_device(
    queries,
    key_page_cache,
    value_page_cache,
    shard_page_index,
    sequence_page_count,
    last_page_tokens,
    sequence_adapter_entry,
    batch_adapters,
    output_projection_weight,
    adapter_down_weight,
    adapter_up_weight,
):
    rows, width = queries.shape
    peers = lax.axis_size("batch")
    heads = lax.axis_size("head")
    stored, _, rank = adapter_down_weight.shape
    output_width = adapter_up_weight.shape[2]
    pages = key_page_cache.shape[0]
    tokens = pages * PAGE
    slots = peers * BLOCK
    query_rows = rows * (HQ // KVH)

    send, attention, target = call(
        functools.partial(source_kernel, stored=stored, peers=peers),
        [((slots, width), BF16), ((rows, width), BF16), ((1, rows), I32)],
        [
            shard_page_index,
            sequence_page_count,
            last_page_tokens.reshape(1, rows),
            sequence_adapter_entry.reshape(1, rows),
            batch_adapters,
            queries,
            key_page_cache.reshape(tokens, HD),
            value_page_cache.reshape(tokens, HD),
        ],
        scratch=[
            pltpu.VMEM((1, pages), I32),
            pltpu.VMEM((1, rows), I32),
            pltpu.VMEM((1, rows), I32),
            pltpu.VMEM((1, rows), I32),
            pltpu.VMEM((1, batch_adapters.shape[1]), I32),
            pltpu.VMEM((rows, width), BF16),
            pltpu.VMEM((tokens, HD), BF16),
            pltpu.VMEM((tokens, HD), BF16),
            pltpu.VMEM((query_rows, tokens), F32),
            pltpu.VMEM((tokens // 128, 128), F32),
            pltpu.SemaphoreType.DMA((7 + PIECES,)),
        ],
        hbm=range(8),
        mib=60,
        flops=4 * query_rows * tokens * HD,
    )
    got = exchange(send.reshape(peers, BLOCK, width), "batch").reshape(slots, width)

    half = rows // 2
    core = (lax.axis_index("head") & 1).astype(I32).reshape(1, 1)
    base_block = pl.BlockSpec((1, half, output_width), lambda h: (h, 0, 0))
    keep, give = pl.pallas_call(
        base_kernel,
        grid=(heads,),
        out_shape=[jax.ShapeDtypeStruct((heads, half, output_width), BF16)] * 2,
        in_specs=[
            pl.BlockSpec(memory_space=pltpu.SMEM),
            pl.BlockSpec((rows, width), lambda h: (0, 0)),
            pl.BlockSpec((width, output_width), lambda h: (0, h)),
        ],
        out_specs=[base_block, base_block],
        cost_estimate=pl.CostEstimate(
            flops=2 * rows * width * heads * output_width, transcendentals=0, bytes_accessed=5 << 20
        ),
        compiler_params=pltpu.CompilerParams(vmem_limit_bytes=8 << 20),
    )(core, attention, output_projection_weight)
    sibling = lax.ppermute(give, "head", [(h, h ^ 1) for h in range(heads)])

    wide = output_width + 2 * HOME_ROWS
    parts, closing, local, over = call(
        home_down_kernel,
        [((heads, half, wide), BF16), ((HOME_ROWS, slots), BF16), ((HOME_ROWS, HOME_ROWS), F32), ((8, 128), F32)],
        [got, jnp.swapaxes(adapter_down_weight, 1, 2).reshape(stored * rank, width), keep, sibling],
        flops=2 * HOME_ROWS * width * stored * rank,
    )
    parts = exchange(parts, "head")
    (back,) = call(
        home_up_kernel,
        [((slots, output_width), BF16)],
        [parts, adapter_up_weight.reshape(stored * rank, output_width), closing, local, over],
        flops=2 * HOME_ROWS * output_width * stored * rank,
    )
    back = exchange(back.reshape(peers, BLOCK, output_width), "batch").reshape(slots, output_width)
    out, base, over = call(
        tail_kernel,
        [((rows, output_width), BF16), ((rows, output_width), F32), ((1, 1), I32)],
        [back, parts, target],
        smem_out=(2,),
        flops=2 * rows * slots * output_width,
    )

    def moving():
        grown = grown_by_moving_maps(
            attention, sequence_adapter_entry, batch_adapters, adapter_down_weight, adapter_up_weight
        )
        return (base + grown).astype(BF16)

    return lax.switch(over[0, 0], [lambda: out, moving])


def solution(mesh):
    in_specs = (
        P("batch", "head"),
        P("batch", None, "head"),
        P("batch", None, "head"),
        P("batch", None),
        P("batch", None),
        P("batch"),
        P("batch"),
        P("batch", None),
        P("head", None),
        P("batch", "head", None),
        P("batch", None, "head"),
    )
    out_specs = P("batch", "head")
    return jax.shard_map(
        per_device, mesh=mesh, in_specs=in_specs, out_specs=out_specs, check_vma=False
    )
```

```python
import functools

import jax
import jax.numpy as jnp
from jax import lax
from jax.experimental import pallas as pl
from jax.experimental.pallas import tpu as pltpu
from jax.sharding import PartitionSpec as P

HQ = 32
KVH = 8
HD = 128
PAGE = 16
BLOCK = 16
HOME_ROWS = 128
CHUNK = 512
PIECES = 4
F32, BF16, I32 = jnp.float32, jnp.bfloat16, jnp.int32


def iota(shape, dim):
    return lax.broadcasted_iota(I32, shape, dim)


def nn(a, b):
    return lax.dot_general(a, b, (((1,), (0,)), ((), ())), preferred_element_type=F32)


def nt(a, b):
    return lax.dot_general(a, b, (((1,), (1,)), ((), ())), preferred_element_type=F32)


def column(row):
    n = row.shape[1]
    return jnp.sum(jnp.where(iota((n, n), 0) == iota((n, n), 1), row, 0.0), axis=1, keepdims=True)


def source_kernel(
    index_hbm,
    count_hbm,
    last_hbm,
    entry_hbm,
    list_hbm,
    q_hbm,
    keys_hbm,
    values_hbm,
    send_ref,
    attention_ref,
    target_ref,
    index_ref,
    count_ref,
    last_ref,
    entry_ref,
    list_ref,
    q_ref,
    keys_ref,
    values_ref,
    scores_ref,
    owner_ref,
    sems,
    *,
    stored,
    peers,
):
    rows = q_ref.shape[0]
    pages = index_ref.shape[1]
    tokens = pages * PAGE
    groups = HQ // KVH
    steps = tokens // CHUNK
    piece = tokens // PIECES
    small = [
        pltpu.make_async_copy(source, target, sems.at[n])
        for n, (source, target) in enumerate(
            [
                (count_hbm, count_ref),
                (last_hbm, last_ref),
                (index_hbm, index_ref),
                (entry_hbm, entry_ref),
                (list_hbm, list_ref),
                (q_hbm, q_ref),
            ]
        )
    ]
    copy_keys = [
        pltpu.make_async_copy(
            keys_hbm.at[pl.ds(n * piece, piece)], keys_ref.at[pl.ds(n * piece, piece)], sems.at[6 + n]
        )
        for n in range(PIECES)
    ]
    copy_values = pltpu.make_async_copy(values_hbm, values_ref, sems.at[6 + PIECES])
    for copy in small:
        copy.start()
    for copy in copy_keys:
        copy.start()
    copy_values.start()
    for copy in small:
        copy.wait()

    count = count_ref[...].astype(F32)
    end = jnp.sum(jnp.where(iota((rows, rows), 1) <= iota((rows, rows), 0), count, 0.0), axis=1, keepdims=True)
    last = column(last_ref[...].astype(F32))
    position = iota((rows, pages), 1).astype(F32)
    owner = jnp.sum((end <= position).astype(F32), axis=0, keepdims=True)
    limit = PAGE - jnp.sum(jnp.where(position == end - 1.0, PAGE - last, 0.0), axis=0, keepdims=True)
    index = index_ref[...]
    per_row = 128 // PAGE
    high = iota((tokens // 128, pages), 0) == index // per_row
    low = (iota((128, pages), 0) // PAGE == index % per_row).astype(F32).astype(BF16)
    owner = nt(jnp.where(high, owner, 0.0).astype(BF16), low)
    limit = nt(jnp.where(high, limit, 0.0).astype(BF16), low)
    inside = (iota((tokens // 128, 128), 1) % PAGE).astype(F32) < limit
    owner_ref[...] = jnp.where(inside, owner, -1.0)

    adapters = list_ref[...].astype(F32)
    entry = entry_ref[...].astype(F32)
    need = adapters.shape[1]
    ids_row = jnp.sum(
        jnp.where(iota((need, rows), 0).astype(F32) == entry, column(adapters), 0.0), axis=0, keepdims=True
    )
    ids_col = column(ids_row)
    home_row = ids_row.astype(I32) // stored
    home_col = ids_col.astype(I32) // stored
    local_row = ids_row.astype(I32) % stored
    same = home_col == home_row
    sub, lane = iota((rows, rows), 0), iota((rows, rows), 1)
    place_row = jnp.sum((same & (sub < lane)).astype(F32), axis=0, keepdims=True).astype(I32)
    place_col = jnp.sum((same & (lane < sub)).astype(F32), axis=1, keepdims=True).astype(I32)
    target = jnp.where(place_row < BLOCK - 1, home_row * BLOCK + place_row, -1)
    target_ref[...] = target
    over = jnp.max(place_row.astype(F32), axis=1, keepdims=True) >= BLOCK - 1
    width = q_ref.shape[1]
    heads_of = jnp.where(iota((peers, rows), 0) == home_row, local_row + 1, 0).astype(F32).astype(BF16)
    spread = (iota((rows, width), 1) % BLOCK == place_col).astype(F32).astype(BF16)
    header = nn(heads_of, spread)
    header = jnp.where(iota((peers, width), 1) % BLOCK == BLOCK - 1, over.astype(F32), header).astype(BF16)

    q = jnp.concatenate([q_ref[:, g * HD : (g + 1) * HD] for g in range(groups)], axis=0)
    own = (iota((groups * rows, 128), 0) % rows).astype(F32)
    top = jnp.full((groups * rows, 128), -1e30, F32)
    for step in range(steps):
        if step * CHUNK % piece == 0:
            copy_keys[step * CHUNK // piece].wait()
        block = nt(q, keys_ref[step * CHUNK : (step + 1) * CHUNK, :])
        for part in range(CHUNK // 128):
            at = step * (CHUNK // 128) + part
            kept = jnp.where(owner_ref[at : at + 1, :] == own, block[:, part * 128 : (part + 1) * 128], -1e30)
            scores_ref[:, at * 128 : (at + 1) * 128] = kept
            top = jnp.maximum(top, kept)
    factor = HD**-0.5 * 1.4426950408889634
    top = jnp.max(top, axis=1, keepdims=True)
    copy_values.wait()
    total = jnp.zeros((groups * rows, 128), F32)
    mixed = jnp.zeros((groups * rows, HD), F32)
    for step in range(steps):
        powers = jnp.exp2((scores_ref[:, step * CHUNK : (step + 1) * CHUNK] - top) * factor)
        for part in range(CHUNK // 128):
            total = total + powers[:, part * 128 : (part + 1) * 128]
        mixed = mixed + nn(powers.astype(BF16), values_ref[step * CHUNK : (step + 1) * CHUNK, :])
    mixed = (mixed / jnp.sum(total, axis=1, keepdims=True)).astype(BF16)
    attention = jnp.concatenate([mixed[g * rows : (g + 1) * rows] for g in range(groups)], axis=1)
    attention_ref[...] = attention

    slots = peers * BLOCK
    picked = jnp.concatenate(
        [
            (iota((slots, rows), 0) == target).astype(F32),
            (iota((slots, peers), 0) == iota((slots, peers), 1) * BLOCK + BLOCK - 1).astype(F32),
        ],
        axis=1,
    ).astype(BF16)
    send_ref[...] = nn(picked, jnp.concatenate([attention, header], axis=0)).astype(BF16)


def base_kernel(place_ref, attention_ref, weight_ref, keep_ref, give_ref):
    heads, half, output_width = keep_ref.shape
    first = place_ref[0, 0] == 0
    attention = attention_ref[...]
    for h in range(heads):
        product = nn(attention, weight_ref[:, h * output_width : (h + 1) * output_width])
        keep_ref[h] = jnp.where(first, product[:half], product[half:]).astype(BF16)
        give_ref[h] = jnp.where(first, product[half:], product[:half]).astype(BF16)


def pair_kernel(place_ref, keep_ref, sibling_ref, keep_out_ref, give_out_ref):
    heads, quarter, _ = keep_out_ref.shape
    first = place_ref[0, 1] == 0
    for h in range(heads):
        both = keep_ref[h].astype(F32) + sibling_ref[h].astype(F32)
        keep_out_ref[h] = jnp.where(first, both[:quarter], both[quarter:]).astype(BF16)
        give_out_ref[h] = jnp.where(first, both[quarter:], both[:quarter]).astype(BF16)


def home_down_kernel(got_ref, down_ref, keep_ref, other_ref, parts_ref, closing_ref, local_ref, over_ref):
    slots, width = got_ref.shape
    peers = slots // BLOCK
    got = got_ref[...]
    is_header = (iota((peers, slots), 1) == iota((peers, slots), 0) * BLOCK + BLOCK - 1).astype(F32).astype(BF16)
    header = nn(is_header, got)[:, :slots]
    lane = iota((peers, slots), 1)
    sub = iota((peers, slots), 0)
    flags = jnp.where(lane % BLOCK == BLOCK - 1, header, 0.0)
    ids = jnp.where(lane % BLOCK == BLOCK - 1, 0.0, header)
    ids_first = jnp.where(lane < BLOCK, ids, 0.0)
    filled = jnp.sum((ids_first > 0.0).astype(F32), axis=1, keepdims=True)
    before = jnp.sum(jnp.where(sub < lane // BLOCK, filled, 0.0), axis=0, keepdims=True)
    here = jnp.sum(jnp.where(sub == lane // BLOCK, filled, 0.0), axis=0, keepdims=True)
    local = jnp.sum(jnp.where(sub == lane // BLOCK, ids, 0.0), axis=0, keepdims=True)
    within = (iota((1, slots), 1) % BLOCK).astype(F32)
    at = jnp.where(within < here, before + within, -1.0)
    closing = (at == iota((HOME_ROWS, slots), 0).astype(F32)).astype(F32).astype(BF16)
    closing_ref[...] = closing
    closed = nn(closing, got).astype(BF16)
    locals_ = jnp.broadcast_to(local, (HOME_ROWS, slots)).astype(BF16)
    local_ref[...] = nt(closing, locals_)
    local_lanes = nt(locals_, closing)[:1, :]
    per_map = nt(down_ref[...], closed)
    rank = per_map.shape[0] // 16
    total = jnp.zeros((rank, HOME_ROWS), F32)
    for n in range(16):
        total = total + jnp.where(local_lanes == n + 1.0, per_map[n * rank : (n + 1) * rank, :], 0.0)
    total = total.astype(BF16)
    heads, quarter, output_width = keep_ref.shape
    total = jnp.concatenate([total[n * quarter : (n + 1) * quarter] for n in range(4)], axis=1)
    for h in range(heads):
        both = keep_ref[h].astype(F32) + other_ref[h].astype(F32)
        parts_ref[h, :, :output_width] = both.astype(BF16)
        parts_ref[h, :, output_width:] = total
    any_pair = jnp.max(jnp.max(flags, axis=1, keepdims=True), axis=0, keepdims=True)
    served = jnp.sum(filled, axis=0, keepdims=True)
    over = jnp.maximum(any_pair, (served > HOME_ROWS).astype(F32))
    over_ref[...] = jnp.broadcast_to(over, over_ref.shape)


def home_up_kernel(parts_ref, up_ref, closing_ref, local_ref, over_ref, back_ref):
    heads, quarter, wide = parts_ref.shape
    rank = 4 * quarter
    width = wide - 4 * HOME_ROWS
    slots = closing_ref.shape[1]
    total = parts_ref[0, :, width:].astype(F32)
    for h in range(1, heads):
        total = total + parts_ref[h, :, width:].astype(F32)
    total = jnp.concatenate([total[:, n * HOME_ROWS : (n + 1) * HOME_ROWS] for n in range(4)], axis=0)
    ranked = jnp.concatenate([total, total], axis=0).T
    local = local_ref[...]
    stored = up_ref.shape[0] // rank
    side = iota((HOME_ROWS, 128), 1) // rank
    spread = jnp.concatenate(
        [jnp.where(local == (side + 2 * pair + 1).astype(F32), ranked, 0.0).astype(BF16) for pair in range(stored // 2)],
        axis=1,
    )
    grown = nn(spread, up_ref[...]).astype(BF16)
    opened = closing_ref[...].astype(F32).T.astype(BF16)
    back = nn(opened, grown)
    row = iota((slots, width), 0)
    back_ref[...] = jnp.where(row % BLOCK == BLOCK - 1, over_ref[:1, :1], back).astype(BF16)


def tail_kernel(back_ref, parts_ref, target_ref, out_ref, base_ref, over_ref):
    heads = parts_ref.shape[0]
    rows = target_ref.shape[1]
    slots, width = back_ref.shape
    base = [
        parts_ref[2 * side + core, :, :width].astype(F32) + parts_ref[heads // 2 + 2 * side + core, :, :width].astype(F32)
        for core in range(2)
        for side in range(2)
    ]
    base = jnp.concatenate(base, axis=0)
    target = column(target_ref[...].astype(F32))
    picked = (iota((rows, slots), 1).astype(F32) == target).astype(F32).astype(BF16)
    back = back_ref[...]
    out_ref[...] = (base + nn(picked, back)).astype(BF16)
    base_ref[...] = base
    peers = slots // BLOCK
    is_header = (iota((peers, slots), 1) == iota((peers, slots), 0) * BLOCK + BLOCK - 1).astype(F32).astype(BF16)
    over_ref[0, 0] = (jnp.max(nn(is_header, back[:, :128])) > 0.0).astype(I32)


def call(body, outs, args, scratch=(), hbm=(), smem=(), smem_out=(), flops=0, mib=8):
    def spec(n, in_hbm, in_smem):
        space = pltpu.HBM if n in in_hbm else pltpu.SMEM if n in in_smem else pltpu.VMEM
        return pl.BlockSpec(memory_space=space)

    return pl.pallas_call(
        body,
        out_shape=[jax.ShapeDtypeStruct(shape, kind) for shape, kind in outs],
        in_specs=[spec(n, hbm, smem) for n in range(len(args))],
        out_specs=[spec(n, (), smem_out) for n in range(len(outs))],
        scratch_shapes=list(scratch),
        cost_estimate=pl.CostEstimate(flops=flops, transcendentals=0, bytes_accessed=1 << 20),
        compiler_params=pltpu.CompilerParams(vmem_limit_bytes=mib << 20),
    )(*args)


def from_everyone(shard, axis):
    count = lax.axis_size(axis)
    return lax.all_to_all(
        jnp.broadcast_to(shard[None], (count, *shard.shape)), axis, 0, 0, tiled=True
    )


def joined_along(blocks, dim):
    blocks = jnp.moveaxis(blocks, 0, dim)
    dims = blocks.shape
    return blocks.reshape(*dims[:dim], dims[dim] * dims[dim + 1], *dims[dim + 2 :])


def collect(shard, axis, dim):
    blocks = from_everyone(shard, axis)
    return joined_along(blocks, dim)


def exchange(blocks, axis):
    return lax.all_to_all(blocks, axis, split_axis=0, concat_axis=0, tiled=True)


def grown_by_moving_maps(
    attention, sequence_adapter_entry, batch_adapters, adapter_down_weight, adapter_up_weight
):
    rows = attention.shape[0]
    my_index = lax.axis_index("batch")
    peers = lax.axis_size("batch")
    count_each_shard = adapter_down_weight.shape[0]
    adapter_rank_width = adapter_down_weight.shape[2]
    output_width = adapter_up_weight.shape[2]
    need = batch_adapters.shape[1]
    own_list = batch_adapters[0]
    slot_match = sequence_adapter_entry[:, None] == jnp.arange(need, dtype=jnp.int32)[None, :]
    lists = collect(batch_adapters, "batch", 0)
    slot_cap = 2 * need // peers
    mine = (lists // count_each_shard == my_index).astype(jnp.int32)
    before = jnp.cumsum(mine, axis=1) - mine
    slot_range = jnp.arange(slot_cap, dtype=jnp.int32)
    select = (mine[:, None, :] == 1) & (before[:, None, :] == slot_range[None, :, None])
    shard_local_numbers = jnp.sum(
        jnp.where(select, (lists % count_each_shard)[:, None, :], 0), axis=-1
    )
    filled = jnp.any(select, axis=-1)
    stored_range = jnp.arange(count_each_shard, dtype=jnp.int32)
    one_hot = (
        (shard_local_numbers[:, :, None] == stored_range[None, None, :]) & filled[:, :, None]
    ).astype(jnp.bfloat16)
    send_shrink = jnp.einsum(
        "bcn,nkr->bckr", one_hot, adapter_down_weight, preferred_element_type=jnp.float32
    ).astype(jnp.bfloat16)
    send_expand = jnp.einsum(
        "bcn,nrw->bcrw", one_hot, adapter_up_weight, preferred_element_type=jnp.float32
    ).astype(jnp.bfloat16)
    got_shrink, got_expand = exchange(send_shrink, "batch"), exchange(send_expand, "batch")
    my_home = own_list // count_each_shard
    order_range = jnp.arange(need, dtype=jnp.int32)
    same_home = (my_home[:, None] == my_home[None, :]) & (
        order_range[None, :] < order_range[:, None]
    )
    arrival = my_home * slot_cap + jnp.sum(same_home, axis=1)
    seq_arrival = jnp.sum(jnp.where(slot_match, arrival[None, :], 0), axis=1)
    total_slots = peers * slot_cap
    picked = seq_arrival[:, None] == jnp.arange(total_slots, dtype=jnp.int32)[None, :]
    flat_shrink = got_shrink.reshape(total_slots, got_shrink.shape[2], adapter_rank_width)
    per_slot = jnp.einsum("sk,nkr->snr", attention, flat_shrink, preferred_element_type=jnp.float32)
    shrink_part = jnp.sum(per_slot * picked.astype(jnp.float32)[:, :, None], axis=1)
    ranked = lax.psum(shrink_part, "head").astype(jnp.bfloat16)
    spread = (ranked[:, None, :] * picked.astype(jnp.bfloat16)[:, :, None]).reshape(
        rows, total_slots * adapter_rank_width
    )
    return jnp.dot(
        spread,
        got_expand.reshape(total_slots * adapter_rank_width, output_width),
        preferred_element_type=jnp.float32,
    )


def per_device(
    queries,
    key_page_cache,
    value_page_cache,
    shard_page_index,
    sequence_page_count,
    last_page_tokens,
    sequence_adapter_entry,
    batch_adapters,
    output_projection_weight,
    adapter_down_weight,
    adapter_up_weight,
):
    rows, width = queries.shape
    peers = lax.axis_size("batch")
    heads = lax.axis_size("head")
    stored, _, rank = adapter_down_weight.shape
    output_width = adapter_up_weight.shape[2]
    pages = key_page_cache.shape[0]
    tokens = pages * PAGE
    slots = peers * BLOCK
    query_rows = rows * (HQ // KVH)

    send, attention, target = call(
        functools.partial(source_kernel, stored=stored, peers=peers),
        [((slots, width), BF16), ((rows, width), BF16), ((1, rows), I32)],
        [
            shard_page_index,
            sequence_page_count,
            last_page_tokens.reshape(1, rows),
            sequence_adapter_entry.reshape(1, rows),
            batch_adapters,
            queries,
            key_page_cache.reshape(tokens, HD),
            value_page_cache.reshape(tokens, HD),
        ],
        scratch=[
            pltpu.VMEM((1, pages), I32),
            pltpu.VMEM((1, rows), I32),
            pltpu.VMEM((1, rows), I32),
            pltpu.VMEM((1, rows), I32),
            pltpu.VMEM((1, batch_adapters.shape[1]), I32),
            pltpu.VMEM((rows, width), BF16),
            pltpu.VMEM((tokens, HD), BF16),
            pltpu.VMEM((tokens, HD), BF16),
            pltpu.VMEM((query_rows, tokens), F32),
            pltpu.VMEM((tokens // 128, 128), F32),
            pltpu.SemaphoreType.DMA((7 + PIECES,)),
        ],
        hbm=range(8),
        mib=60,
        flops=4 * query_rows * tokens * HD,
    )
    got = exchange(send.reshape(peers, BLOCK, width), "batch").reshape(slots, width)

    half, quarter = rows // 2, rows // 4
    head = lax.axis_index("head").astype(I32)
    place = jnp.stack([head & 1, (head >> 1) & 1]).reshape(1, 2)
    keep, give = call(
        base_kernel,
        [((heads, half, output_width), BF16)] * 2,
        [place, attention, output_projection_weight],
        smem=(0,),
        flops=2 * rows * width * heads * output_width,
        mib=12,
    )
    sibling = lax.ppermute(give, "head", [(h, h ^ 1) for h in range(heads)])
    keep, give = call(
        pair_kernel, [((heads, quarter, output_width), BF16)] * 2, [place, keep, sibling], smem=(0,), flops=1 << 20
    )
    other = lax.ppermute(give, "head", [(h, h ^ 2) for h in range(heads)])

    wide = output_width + 4 * HOME_ROWS
    parts, closing, local, over = call(
        home_down_kernel,
        [((heads, quarter, wide), BF16), ((HOME_ROWS, slots), BF16), ((HOME_ROWS, HOME_ROWS), F32), ((8, 128), F32)],
        [got, jnp.swapaxes(adapter_down_weight, 1, 2).reshape(stored * rank, width), keep, other],
        flops=2 * HOME_ROWS * width * stored * rank,
    )
    parts = exchange(parts, "head")
    (back,) = call(
        home_up_kernel,
        [((slots, output_width), BF16)],
        [parts, adapter_up_weight.reshape(stored * rank, output_width), closing, local, over],
        flops=2 * HOME_ROWS * output_width * stored * rank,
    )
    back = exchange(back.reshape(peers, BLOCK, output_width), "batch").reshape(slots, output_width)
    out, base, over = call(
        tail_kernel,
        [((rows, output_width), BF16), ((rows, output_width), F32), ((1, 1), I32)],
        [back, parts, target],
        smem_out=(2,),
        flops=2 * rows * slots * output_width,
    )

    def moving():
        grown = grown_by_moving_maps(
            attention, sequence_adapter_entry, batch_adapters, adapter_down_weight, adapter_up_weight
        )
        return (base + grown).astype(BF16)

    return lax.switch(over[0, 0], [lambda: out, moving])


def solution(mesh):
    in_specs = (
        P("batch", "head"),
        P("batch", None, "head"),
        P("batch", None, "head"),
        P("batch", None),
        P("batch", None),
        P("batch"),
        P("batch"),
        P("batch", None),
        P("head", None),
        P("batch", "head", None),
        P("batch", None, "head"),
    )
    out_specs = P("batch", "head")
    return jax.shard_map(
        per_device, mesh=mesh, in_specs=in_specs, out_specs=out_specs, check_vma=False
    )
```

```python
import functools

import jax
import jax.numpy as jnp
from jax import lax
from jax.experimental import pallas as pl
from jax.experimental.pallas import tpu as pltpu
from jax.sharding import PartitionSpec as P

HQ = 32
KVH = 8
HD = 128
PAGE = 16
BLOCK = 16
HOME_ROWS = 128
CHUNK = 512
PIECES = 4
F32, BF16, I32 = jnp.float32, jnp.bfloat16, jnp.int32


def iota(shape, dim):
    return lax.broadcasted_iota(I32, shape, dim)


def nn(a, b):
    return lax.dot_general(a, b, (((1,), (0,)), ((), ())), preferred_element_type=F32)


def nt(a, b):
    return lax.dot_general(a, b, (((1,), (1,)), ((), ())), preferred_element_type=F32)


def column(row):
    n = row.shape[1]
    return jnp.sum(jnp.where(iota((n, n), 0) == iota((n, n), 1), row, 0.0), axis=1, keepdims=True)


def source_kernel(
    index_hbm,
    count_hbm,
    last_hbm,
    entry_hbm,
    list_hbm,
    q_hbm,
    keys_hbm,
    values_hbm,
    send_ref,
    attention_ref,
    target_ref,
    index_ref,
    count_ref,
    last_ref,
    entry_ref,
    list_ref,
    q_ref,
    keys_ref,
    values_ref,
    scores_ref,
    owner_ref,
    sems,
    *,
    stored,
    peers,
):
    rows = q_ref.shape[0]
    pages = index_ref.shape[1]
    tokens = pages * PAGE
    groups = HQ // KVH
    steps = tokens // CHUNK
    piece = tokens // PIECES
    small = [
        pltpu.make_async_copy(source, target, sems.at[n])
        for n, (source, target) in enumerate(
            [
                (count_hbm, count_ref),
                (last_hbm, last_ref),
                (index_hbm, index_ref),
                (entry_hbm, entry_ref),
                (list_hbm, list_ref),
                (q_hbm, q_ref),
            ]
        )
    ]
    copy_keys = [
        pltpu.make_async_copy(
            keys_hbm.at[pl.ds(n * piece, piece)], keys_ref.at[pl.ds(n * piece, piece)], sems.at[6 + n]
        )
        for n in range(PIECES)
    ]
    copy_values = pltpu.make_async_copy(values_hbm, values_ref, sems.at[6 + PIECES])
    for copy in small:
        copy.start()
    for copy in copy_keys:
        copy.start()
    copy_values.start()
    for copy in small:
        copy.wait()

    count = count_ref[...].astype(F32)
    end = jnp.sum(jnp.where(iota((rows, rows), 1) <= iota((rows, rows), 0), count, 0.0), axis=1, keepdims=True)
    last = column(last_ref[...].astype(F32))
    position = iota((rows, pages), 1).astype(F32)
    owner = jnp.sum((end <= position).astype(F32), axis=0, keepdims=True)
    limit = PAGE - jnp.sum(jnp.where(position == end - 1.0, PAGE - last, 0.0), axis=0, keepdims=True)
    index = index_ref[...]
    per_row = 128 // PAGE
    high = iota((tokens // 128, pages), 0) == index // per_row
    low = (iota((128, pages), 0) // PAGE == index % per_row).astype(F32).astype(BF16)
    owner = nt(jnp.where(high, owner, 0.0).astype(BF16), low)
    limit = nt(jnp.where(high, limit, 0.0).astype(BF16), low)
    inside = (iota((tokens // 128, 128), 1) % PAGE).astype(F32) < limit
    owner_ref[...] = jnp.where(inside, owner, -1.0)

    adapters = list_ref[...].astype(F32)
    entry = entry_ref[...].astype(F32)
    need = adapters.shape[1]
    ids_row = jnp.sum(
        jnp.where(iota((need, rows), 0).astype(F32) == entry, column(adapters), 0.0), axis=0, keepdims=True
    )
    ids_col = column(ids_row)
    home_row = ids_row.astype(I32) // stored
    home_col = ids_col.astype(I32) // stored
    local_row = ids_row.astype(I32) % stored
    same = home_col == home_row
    sub, lane = iota((rows, rows), 0), iota((rows, rows), 1)
    place_row = jnp.sum((same & (sub < lane)).astype(F32), axis=0, keepdims=True).astype(I32)
    place_col = jnp.sum((same & (lane < sub)).astype(F32), axis=1, keepdims=True).astype(I32)
    target = jnp.where(place_row < BLOCK - 1, home_row * BLOCK + place_row, -1)
    target_ref[...] = target
    over = jnp.max(place_row.astype(F32), axis=1, keepdims=True) >= BLOCK - 1
    width = q_ref.shape[1]
    heads_of = jnp.where(iota((peers, rows), 0) == home_row, local_row + 1, 0).astype(F32).astype(BF16)
    spread = (iota((rows, width), 1) % BLOCK == place_col).astype(F32).astype(BF16)
    header = nn(heads_of, spread)
    header = jnp.where(iota((peers, width), 1) % BLOCK == BLOCK - 1, over.astype(F32), header).astype(BF16)

    q = jnp.concatenate([q_ref[:, g * HD : (g + 1) * HD] for g in range(groups)], axis=0)
    own = (iota((groups * rows, 128), 0) % rows).astype(F32)
    top = jnp.full((groups * rows, 128), -1e30, F32)
    for step in range(steps):
        if step * CHUNK % piece == 0:
            copy_keys[step * CHUNK // piece].wait()
        block = nt(q, keys_ref[step * CHUNK : (step + 1) * CHUNK, :])
        for part in range(CHUNK // 128):
            at = step * (CHUNK // 128) + part
            kept = jnp.where(owner_ref[at : at + 1, :] == own, block[:, part * 128 : (part + 1) * 128], -1e30)
            scores_ref[:, at * 128 : (at + 1) * 128] = kept
            top = jnp.maximum(top, kept)
    factor = HD**-0.5 * 1.4426950408889634
    top = jnp.max(top, axis=1, keepdims=True)
    copy_values.wait()
    total = jnp.zeros((groups * rows, 128), F32)
    mixed = jnp.zeros((groups * rows, HD), F32)
    for step in range(steps):
        powers = jnp.exp2((scores_ref[:, step * CHUNK : (step + 1) * CHUNK] - top) * factor)
        for part in range(CHUNK // 128):
            total = total + powers[:, part * 128 : (part + 1) * 128]
        mixed = mixed + nn(powers.astype(BF16), values_ref[step * CHUNK : (step + 1) * CHUNK, :])
    mixed = (mixed / jnp.sum(total, axis=1, keepdims=True)).astype(BF16)
    attention = jnp.concatenate([mixed[g * rows : (g + 1) * rows] for g in range(groups)], axis=1)
    attention_ref[...] = attention

    slots = peers * BLOCK
    picked = jnp.concatenate(
        [
            (iota((slots, rows), 0) == target).astype(F32),
            (iota((slots, peers), 0) == iota((slots, peers), 1) * BLOCK + BLOCK - 1).astype(F32),
        ],
        axis=1,
    ).astype(BF16)
    send_ref[...] = nn(picked, jnp.concatenate([attention, header], axis=0)).astype(BF16)


def base_kernel(place_ref, attention_ref, weight_ref, keep_ref, give_ref):
    count, _, output_width = keep_ref.shape
    first = place_ref[0, 0] == 0
    attention = attention_ref[...]
    for n in range(count):
        one = nn(attention, weight_ref[:, 2 * n * output_width : (2 * n + 1) * output_width])
        two = nn(attention, weight_ref[:, (2 * n + 1) * output_width : (2 * n + 2) * output_width])
        keep_ref[n] = jnp.where(first, one, two).astype(BF16)
        give_ref[n] = jnp.where(first, two, one).astype(BF16)


def pair_kernel(place_ref, keep_ref, sibling_ref, keep_out_ref, give_out_ref):
    count = keep_out_ref.shape[0]
    first = place_ref[0, 1] == 0
    for n in range(count):
        one = keep_ref[2 * n].astype(F32) + sibling_ref[2 * n].astype(F32)
        two = keep_ref[2 * n + 1].astype(F32) + sibling_ref[2 * n + 1].astype(F32)
        keep_out_ref[n] = jnp.where(first, one, two).astype(BF16)
        give_out_ref[n] = jnp.where(first, two, one).astype(BF16)


def home_down_kernel(
    place_ref, got_ref, down_ref, keep_ref, other_ref, part_ref, keep_out_ref, give_out_ref, closing_ref, local_ref, over_ref
):
    slots, width = got_ref.shape
    peers = slots // BLOCK
    got = got_ref[...]
    is_header = (iota((peers, slots), 1) == iota((peers, slots), 0) * BLOCK + BLOCK - 1).astype(F32).astype(BF16)
    header = nn(is_header, got)[:, :slots]
    lane = iota((peers, slots), 1)
    sub = iota((peers, slots), 0)
    flags = jnp.where(lane % BLOCK == BLOCK - 1, header, 0.0)
    ids = jnp.where(lane % BLOCK == BLOCK - 1, 0.0, header)
    ids_first = jnp.where(lane < BLOCK, ids, 0.0)
    filled = jnp.sum((ids_first > 0.0).astype(F32), axis=1, keepdims=True)
    before = jnp.sum(jnp.where(sub < lane // BLOCK, filled, 0.0), axis=0, keepdims=True)
    here = jnp.sum(jnp.where(sub == lane // BLOCK, filled, 0.0), axis=0, keepdims=True)
    local = jnp.sum(jnp.where(sub == lane // BLOCK, ids, 0.0), axis=0, keepdims=True)
    within = (iota((1, slots), 1) % BLOCK).astype(F32)
    at = jnp.where(within < here, before + within, -1.0)
    closing = (at == iota((HOME_ROWS, slots), 0).astype(F32)).astype(F32).astype(BF16)
    closing_ref[...] = closing
    closed = nn(closing, got).astype(BF16)
    locals_ = jnp.broadcast_to(local, (HOME_ROWS, slots)).astype(BF16)
    local_ref[...] = nt(closing, locals_)
    local_lanes = nt(locals_, closing)[:1, :]
    per_map = nt(down_ref[...], closed)
    rank = per_map.shape[0] // 16
    total = jnp.zeros((rank, HOME_ROWS), F32)
    for n in range(16):
        total = total + jnp.where(local_lanes == n + 1.0, per_map[n * rank : (n + 1) * rank, :], 0.0)
    part_ref[...] = total
    first = place_ref[0, 2] == 0
    one = keep_ref[0].astype(F32) + other_ref[0].astype(F32)
    two = keep_ref[1].astype(F32) + other_ref[1].astype(F32)
    keep_out_ref[...] = jnp.where(first, one, two)
    give_out_ref[...] = jnp.where(first, two, one).astype(BF16)
    any_pair = jnp.max(jnp.max(flags, axis=1, keepdims=True), axis=0, keepdims=True)
    served = jnp.sum(filled, axis=0, keepdims=True)
    over = jnp.maximum(any_pair, (served > HOME_ROWS).astype(F32))
    over_ref[...] = jnp.broadcast_to(over, over_ref.shape)


def add_kernel(one_ref, two_ref, out_ref):
    out_ref[...] = one_ref[...] + two_ref[...]


def home_up_kernel(one_ref, two_ref, up_ref, closing_ref, local_ref, over_ref, back_ref):
    rank = one_ref.shape[0]
    slots, width = closing_ref.shape[1], up_ref.shape[1]
    total = one_ref[...] + two_ref[...]
    ranked = jnp.concatenate([total, total], axis=0).T
    local = local_ref[...]
    stored = up_ref.shape[0] // rank
    side = iota((HOME_ROWS, 128), 1) // rank
    spread = jnp.concatenate(
        [jnp.where(local == (side + 2 * pair + 1).astype(F32), ranked, 0.0).astype(BF16) for pair in range(stored // 2)],
        axis=1,
    )
    grown = nn(spread, up_ref[...]).astype(BF16)
    opened = closing_ref[...].astype(F32).T.astype(BF16)
    back = nn(opened, grown)
    row = iota((slots, width), 0)
    back_ref[...] = jnp.where(row % BLOCK == BLOCK - 1, over_ref[:1, :1], back).astype(BF16)


def tail_kernel(back_ref, keep_ref, far_ref, target_ref, out_ref, base_ref, over_ref):
    rows = target_ref.shape[1]
    slots, width = back_ref.shape
    base = keep_ref[...] + far_ref[...].astype(F32)
    target = column(target_ref[...].astype(F32))
    picked = (iota((rows, slots), 1).astype(F32) == target).astype(F32).astype(BF16)
    back = back_ref[...]
    out_ref[...] = (base + nn(picked, back)).astype(BF16)
    base_ref[...] = base
    peers = slots // BLOCK
    is_header = (iota((peers, slots), 1) == iota((peers, slots), 0) * BLOCK + BLOCK - 1).astype(F32).astype(BF16)
    over_ref[0, 0] = (jnp.max(nn(is_header, back[:, :128])) > 0.0).astype(I32)


def call(body, outs, args, scratch=(), hbm=(), smem=(), smem_out=(), flops=0, mib=8):
    def spec(n, in_hbm, in_smem):
        space = pltpu.HBM if n in in_hbm else pltpu.SMEM if n in in_smem else pltpu.VMEM
        return pl.BlockSpec(memory_space=space)

    return pl.pallas_call(
        body,
        out_shape=[jax.ShapeDtypeStruct(shape, kind) for shape, kind in outs],
        in_specs=[spec(n, hbm, smem) for n in range(len(args))],
        out_specs=[spec(n, (), smem_out) for n in range(len(outs))],
        scratch_shapes=list(scratch),
        cost_estimate=pl.CostEstimate(flops=flops, transcendentals=0, bytes_accessed=1 << 20),
        compiler_params=pltpu.CompilerParams(vmem_limit_bytes=mib << 20),
    )(*args)


def from_everyone(shard, axis):
    count = lax.axis_size(axis)
    return lax.all_to_all(
        jnp.broadcast_to(shard[None], (count, *shard.shape)), axis, 0, 0, tiled=True
    )


def joined_along(blocks, dim):
    blocks = jnp.moveaxis(blocks, 0, dim)
    dims = blocks.shape
    return blocks.reshape(*dims[:dim], dims[dim] * dims[dim + 1], *dims[dim + 2 :])


def collect(shard, axis, dim):
    blocks = from_everyone(shard, axis)
    return joined_along(blocks, dim)


def exchange(blocks, axis):
    return lax.all_to_all(blocks, axis, split_axis=0, concat_axis=0, tiled=True)


def grown_by_moving_maps(
    attention, sequence_adapter_entry, batch_adapters, adapter_down_weight, adapter_up_weight
):
    rows = attention.shape[0]
    my_index = lax.axis_index("batch")
    peers = lax.axis_size("batch")
    count_each_shard = adapter_down_weight.shape[0]
    adapter_rank_width = adapter_down_weight.shape[2]
    output_width = adapter_up_weight.shape[2]
    need = batch_adapters.shape[1]
    own_list = batch_adapters[0]
    slot_match = sequence_adapter_entry[:, None] == jnp.arange(need, dtype=jnp.int32)[None, :]
    lists = collect(batch_adapters, "batch", 0)
    slot_cap = 2 * need // peers
    mine = (lists // count_each_shard == my_index).astype(jnp.int32)
    before = jnp.cumsum(mine, axis=1) - mine
    slot_range = jnp.arange(slot_cap, dtype=jnp.int32)
    select = (mine[:, None, :] == 1) & (before[:, None, :] == slot_range[None, :, None])
    shard_local_numbers = jnp.sum(
        jnp.where(select, (lists % count_each_shard)[:, None, :], 0), axis=-1
    )
    filled = jnp.any(select, axis=-1)
    stored_range = jnp.arange(count_each_shard, dtype=jnp.int32)
    one_hot = (
        (shard_local_numbers[:, :, None] == stored_range[None, None, :]) & filled[:, :, None]
    ).astype(jnp.bfloat16)
    send_shrink = jnp.einsum(
        "bcn,nkr->bckr", one_hot, adapter_down_weight, preferred_element_type=jnp.float32
    ).astype(jnp.bfloat16)
    send_expand = jnp.einsum(
        "bcn,nrw->bcrw", one_hot, adapter_up_weight, preferred_element_type=jnp.float32
    ).astype(jnp.bfloat16)
    got_shrink, got_expand = exchange(send_shrink, "batch"), exchange(send_expand, "batch")
    my_home = own_list // count_each_shard
    order_range = jnp.arange(need, dtype=jnp.int32)
    same_home = (my_home[:, None] == my_home[None, :]) & (
        order_range[None, :] < order_range[:, None]
    )
    arrival = my_home * slot_cap + jnp.sum(same_home, axis=1)
    seq_arrival = jnp.sum(jnp.where(slot_match, arrival[None, :], 0), axis=1)
    total_slots = peers * slot_cap
    picked = seq_arrival[:, None] == jnp.arange(total_slots, dtype=jnp.int32)[None, :]
    flat_shrink = got_shrink.reshape(total_slots, got_shrink.shape[2], adapter_rank_width)
    per_slot = jnp.einsum("sk,nkr->snr", attention, flat_shrink, preferred_element_type=jnp.float32)
    shrink_part = jnp.sum(per_slot * picked.astype(jnp.float32)[:, :, None], axis=1)
    ranked = lax.psum(shrink_part, "head").astype(jnp.bfloat16)
    spread = (ranked[:, None, :] * picked.astype(jnp.bfloat16)[:, :, None]).reshape(
        rows, total_slots * adapter_rank_width
    )
    return jnp.dot(
        spread,
        got_expand.reshape(total_slots * adapter_rank_width, output_width),
        preferred_element_type=jnp.float32,
    )


def per_device(
    queries,
    key_page_cache,
    value_page_cache,
    shard_page_index,
    sequence_page_count,
    last_page_tokens,
    sequence_adapter_entry,
    batch_adapters,
    output_projection_weight,
    adapter_down_weight,
    adapter_up_weight,
):
    rows, width = queries.shape
    peers = lax.axis_size("batch")
    heads = lax.axis_size("head")
    stored, _, rank = adapter_down_weight.shape
    output_width = adapter_up_weight.shape[2]
    pages = key_page_cache.shape[0]
    tokens = pages * PAGE
    slots = peers * BLOCK
    query_rows = rows * (HQ // KVH)

    send, attention, target = call(
        functools.partial(source_kernel, stored=stored, peers=peers),
        [((slots, width), BF16), ((rows, width), BF16), ((1, rows), I32)],
        [
            shard_page_index,
            sequence_page_count,
            last_page_tokens.reshape(1, rows),
            sequence_adapter_entry.reshape(1, rows),
            batch_adapters,
            queries,
            key_page_cache.reshape(tokens, HD),
            value_page_cache.reshape(tokens, HD),
        ],
        scratch=[
            pltpu.VMEM((1, pages), I32),
            pltpu.VMEM((1, rows), I32),
            pltpu.VMEM((1, rows), I32),
            pltpu.VMEM((1, rows), I32),
            pltpu.VMEM((1, batch_adapters.shape[1]), I32),
            pltpu.VMEM((rows, width), BF16),
            pltpu.VMEM((tokens, HD), BF16),
            pltpu.VMEM((tokens, HD), BF16),
            pltpu.VMEM((query_rows, tokens), F32),
            pltpu.VMEM((tokens // 128, 128), F32),
            pltpu.SemaphoreType.DMA((7 + PIECES,)),
        ],
        hbm=range(8),
        mib=60,
        flops=4 * query_rows * tokens * HD,
    )
    got = exchange(send.reshape(peers, BLOCK, width), "batch").reshape(slots, width)

    head = lax.axis_index("head").astype(I32)
    place = jnp.stack([head & 1, (head >> 1) & 1, (head >> 2) & 1]).reshape(1, 3)
    crossing = [[(h, h ^ bit) for h in range(heads)] for bit in (1, 2, 4)]
    keep, give = call(
        base_kernel,
        [((heads // 2, rows, output_width), BF16)] * 2,
        [place, attention, output_projection_weight],
        smem=(0,),
        flops=2 * rows * width * heads * output_width,
        mib=12,
    )
    sibling = lax.ppermute(give, "head", crossing[0])
    keep, give = call(
        pair_kernel, [((heads // 4, rows, output_width), BF16)] * 2, [place, keep, sibling], smem=(0,), flops=1 << 20
    )
    other = lax.ppermute(give, "head", crossing[1])

    part, keep, give, closing, local, over = call(
        home_down_kernel,
        [
            ((rank, HOME_ROWS), F32),
            ((rows, output_width), F32),
            ((rows, output_width), BF16),
            ((HOME_ROWS, slots), BF16),
            ((HOME_ROWS, HOME_ROWS), F32),
            ((8, 128), F32),
        ],
        [place, got, jnp.swapaxes(adapter_down_weight, 1, 2).reshape(stored * rank, width), keep, other],
        smem=(0,),
        flops=2 * HOME_ROWS * width * stored * rank,
    )
    for bit in range(2):
        (part,) = call(add_kernel, [((rank, HOME_ROWS), F32)], [part, lax.ppermute(part, "head", crossing[bit])])
    last = lax.ppermute(part, "head", crossing[2])
    last, far = lax.optimization_barrier((last, lax.ppermute(give, "head", crossing[2])))
    (back,) = call(
        home_up_kernel,
        [((slots, output_width), BF16)],
        [part, last, adapter_up_weight.reshape(stored * rank, output_width), closing, local, over],
        flops=2 * HOME_ROWS * output_width * stored * rank,
    )
    back = exchange(back.reshape(peers, BLOCK, output_width), "batch").reshape(slots, output_width)
    out, base, over = call(
        tail_kernel,
        [((rows, output_width), BF16), ((rows, output_width), F32), ((1, 1), I32)],
        [back, keep, far, target],
        smem_out=(2,),
        flops=2 * rows * slots * output_width,
    )

    def moving():
        grown = grown_by_moving_maps(
            attention, sequence_adapter_entry, batch_adapters, adapter_down_weight, adapter_up_weight
        )
        return (base + grown).astype(BF16)

    return lax.switch(over[0, 0], [lambda: out, moving])


def solution(mesh):
    in_specs = (
        P("batch", "head"),
        P("batch", None, "head"),
        P("batch", None, "head"),
        P("batch", None),
        P("batch", None),
        P("batch"),
        P("batch"),
        P("batch", None),
        P("head", None),
        P("batch", "head", None),
        P("batch", None, "head"),
    )
    out_specs = P("batch", "head")
    return jax.shard_map(
        per_device, mesh=mesh, in_specs=in_specs, out_specs=out_specs, check_vma=False
    )
```
